256 devices in a mesh: gx: 64 (over x, z, core), gy: 4 (over y).
Axes of the slice: x: 4, y: 4, z: 8, core: 2. Of those that a mesh axis runs over, the one named last changes fastest.
Arguments:
- measures: bfloat16 [2097152, 128], P(('gx', 'gy')), may hold values from -6 to 6
- row_keys: int32 [2097152], P(('gx', 'gy')), may hold values from 0 to 131071, as said below
- orders: bfloat16 [131072, 128], P(('gx', 'gy')), may hold values from -6 to 6
- heavy_keys: int32 [512], replicated, may hold values from 0 to 131071, as said below
- key_slot: int32 [131072], replicated, may hold values from 0 to 131071, as said below
Outputs:
- result: bfloat16 [131072, 128], P(('gx', 'gy'))
- heavy_report: bfloat16 [512, 128], P(('gx', 'gy'))
- slot_rows: float32 [131072], P(('gx', 'gy'))
The draws below stay inside these ranges and needn't reach their ends.
Inputs may be any that keep to these rules, and one draw needn't show every extreme that they name: `heavy_keys`: for each range block d, entries d * 2 to (d + 1) * 2 - 1 are distinct keys of d * 512 to (d + 1) * 512 - 1. `key_slot`: A permutation. Slot s belongs to owner s // 2048 and to quarter (s // 512) % q with q = 4. Key k lies in range block d = k // 512; every range block has exactly 8 keys with slots of each owner, all in quarter d % q. `row_keys`: in the rows of one device, among rows whose key is not heavy, at most 256 have slots of any one owner and at most 64 distinct keys have slots of any one owner; in every device both bounds are reached by some owner.
All inputs are finite; a program needn't handle non-finite values.
Results may differ from the reference program's by a relative error of at most 0.0021.
Values may be sent and summed in bfloat16 or wider, within the bound.
A program may use at most 64 MiB of HBM per device.

```python
import jax
import jax.numpy as jnp
from jax import lax

W = 128
ROWS_DEV = 8192
KEY_DEV = 512
HPD = 2
ROWS = 2097152
KEYS = 131072
HEAVY = 512
OWN_SLOTS = 2048
KPP = 8
CAP = 256
CAPK = 64
N_GX = 64
N_GY = 4
DEVICES = 256


def layout(base):
    seeded = jax.random.fold_in(base, 7)
    first, second, third = jax.random.split(seeded, 3)
    owner_perm = jax.vmap(lambda keyone: jax.random.permutation(keyone, KEY_DEV))(jax.random.split(first, DEVICES))
    device = jnp.arange(DEVICES, dtype=jnp.int32)
    along_x = device // N_GY
    along_y = device % N_GY
    owners = owner_perm // KPP
    within = owner_perm % KPP
    shuffle = jax.vmap(lambda keyone: jax.random.permutation(keyone, KEY_DEV))(jax.random.split(second, N_GX * N_GY))
    shuffle = shuffle.reshape(N_GX, N_GY, KEY_DEV)
    position = shuffle[owners, along_y[:, None], along_x[:, None] * KPP + within]
    key_slot = ((owners * N_GY + along_y[:, None]) * KEY_DEV + position).reshape(KEYS).astype(jnp.int32)
    picked = jax.vmap(lambda keyone: jax.random.permutation(keyone, KEY_DEV)[:HPD])(jax.random.split(third, DEVICES))
    heavy_keys = (device[:, None] * KEY_DEV + picked).reshape(HEAVY).astype(jnp.int32)
    slot_to_key = jnp.argsort(key_slot).astype(jnp.int32)
    heavy_flag = jnp.zeros((KEYS,), jnp.int32).at[heavy_keys].set(1)
    heavy_slot = heavy_flag[slot_to_key]
    return (key_slot, heavy_keys, slot_to_key, heavy_slot)


def draw_key_slot(key, part):
    return layout(key)[0]


def draw_heavy_keys(key, part):
    return layout(key)[1]


def draw_row_keys(key, part):
    key_slot, heavy_keys, slot_to_key, heavy_slot = layout(key)
    seeded = jax.random.fold_in(key, 11)
    favored_pool = jax.random.permutation(jax.random.fold_in(seeded, 3), N_GX)[:max(1, N_GX // 16)]
    tickets = N_GX * CAP
    pool_rank = jnp.where(heavy_slot.reshape(N_GX, OWN_SLOTS) == 1, OWN_SLOTS, 0)

    def one_device(keyone):
        parts = jax.random.split(keyone, 7)
        heavy_count = jax.random.randint(parts[0], (), ROWS_DEV // 4, ROWS_DEV // 2 + 1)
        light_count = ROWS_DEV - heavy_count
        favored = favored_pool[jax.random.randint(parts[1], (), 0, favored_pool.shape[0])]
        ticket_owner = jnp.arange(tickets, dtype=jnp.int32) // CAP
        scores = jnp.where(ticket_owner == favored, 0, tickets) + jax.random.permutation(parts[2], tickets)
        ticket_order = jnp.argsort(scores).astype(jnp.int32)
        row_index = jnp.arange(ROWS_DEV, dtype=jnp.int32)
        chosen = ticket_order[jnp.minimum(row_index, tickets - 1)]
        row_owner = chosen // CAP
        row_ticket = chosen % CAP
        mixing = jax.vmap(lambda keytwo: jax.random.permutation(keytwo, OWN_SLOTS))(jax.random.split(parts[3], N_GX))
        pools = jnp.argsort(pool_rank + mixing, axis=1)[:, :CAPK].astype(jnp.int32)
        spare = jax.random.randint(parts[4], (ROWS_DEV,), 0, CAPK)
        pool_index = jnp.where(row_ticket < CAPK, row_ticket, spare)
        light_keys = slot_to_key[row_owner * OWN_SLOTS + pools[row_owner, pool_index]]
        heavy_pick = heavy_keys[jax.random.randint(parts[5], (ROWS_DEV,), 0, HEAVY)]
        chosen_keys = jnp.where(row_index < light_count, light_keys, heavy_pick)
        return chosen_keys[jax.random.permutation(parts[6], ROWS_DEV)]
    return jax.vmap(one_device)(jax.random.split(seeded, DEVICES)).reshape(ROWS).astype(jnp.int32)


def level_of(own_key, dims, cuts, least, largest):
    factor_of = 1.0
    for dim, shards_of in cuts:
        draws = jax.random.uniform(jax.random.fold_in(jax.random.fold_in(own_key, 6), dim), (shards_of,), jnp.float32, least / len(cuts), largest / len(cuts))
        factor_of = factor_of * jnp.repeat(jnp.exp(draws), dims[dim] // shards_of).reshape((-1,) + (1,) * (len(dims) - 1 - dim))
    return factor_of


def scatter_about(rng, dims, spread, reach, pieces=(), kind=jnp.bfloat16):
    gain = level_of(rng, dims, pieces, -0.22, 0.18) if pieces else 1.0
    drawn = jax.random.normal(rng, dims, jnp.float32) * spread * gain
    return jnp.minimum(jnp.maximum(drawn, -reach), reach).astype(kind)


def setup_inputs(seed: int = 0) -> dict:
    key_list = jax.random.split(jax.random.key(seed), 6)
    return {
        "measures": scatter_about(key_list[0], (ROWS, W), 1.0, 6.0, ((0, 256),)),
        "row_keys": draw_row_keys(jax.random.fold_in(key_list[5], 71), 0),
        "orders": scatter_about(key_list[2], (KEYS, W), 1.0, 6.0, ((0, 256),)),
        "heavy_keys": draw_heavy_keys(jax.random.fold_in(key_list[5], 71), 0),
        "key_slot": draw_key_slot(jax.random.fold_in(key_list[5], 71), 0),
    }


def reference(measures, row_keys, orders, heavy_keys, key_slot):
    blocks = measures.reshape(DEVICES, ROWS_DEV, W)
    block_keys = row_keys.reshape(DEVICES, ROWS_DEV)

    def add_block(running, block_piece):
        block_rows, keys_here = block_piece
        totals = running[0] + jax.ops.segment_sum(block_rows.astype(jnp.float32), keys_here, num_segments=KEYS)
        tallies = running[1] + jax.ops.segment_sum(jnp.ones((ROWS_DEV,), jnp.float32), keys_here, num_segments=KEYS)
        return ((totals, tallies), None)
    start_state = (jnp.zeros((KEYS, W), jnp.float32), jnp.zeros((KEYS,), jnp.float32))
    (sums, counts), unused = lax.scan(add_block, start_state, (blocks, block_keys))
    joined = orders.astype(jnp.float32) * sums * lax.rsqrt(1.0 + counts)[:, None]
    result = joined.astype(jnp.bfloat16)
    heavy_report = joined[heavy_keys].astype(jnp.bfloat16)
    heavy_flag = jnp.zeros((KEYS,), jnp.float32).at[heavy_keys].set(1.0)
    slot_rows = jnp.zeros((KEYS,), jnp.float32).at[key_slot].set(counts * (1.0 - heavy_flag))
    return (result, heavy_report, slot_rows)
```

```python
import functools

import jax
import jax.numpy as jnp
from jax import lax
from jax.experimental import pallas as pl
from jax.experimental.pallas import tpu as pltpu
from jax.sharding import PartitionSpec as P

MESH = pl.DeviceIdType.MESH
LANES = 128
F32 = jnp.float32
BF16 = jnp.bfloat16
I32 = jnp.int32
I16 = jnp.int16
VMEM = pl.BlockSpec(memory_space=pltpu.VMEM)
SMEM = pl.BlockSpec(memory_space=pltpu.SMEM)
LIMIT = 60 * 1024 * 1024
NN = (((1,), (0,)), ((), ()))
NT = (((1,), (1,)), ((), ()))

GX, GY = 64, 4
ROWS = 8192
BLOCK = 2048
CAPK = 64
OWN = 2048
KEY_DEV = 512
KPP = 8
HPD = 2
HPM = HPD * GY
STEPS = 8
CHUNK = STEPS * CAPK
CHUNKS = GX // STEPS
EXTRA = 16
SIDE = 16
MESSAGE = CAPK + SIDE
FULL = 32000.0


def dot(a, b, dims=NN):
    return lax.dot_general(a, b, dims, preferred_element_type=F32)


def iota(shape, dim):
    return lax.broadcasted_iota(I32, shape, dim)


def onehot(mask):
    return jnp.where(mask, 1.0, 0.0).astype(BF16)


def spread16(row):
    wide = jnp.broadcast_to(row, (16, row.shape[1])) - iota((16, row.shape[1]), 0)
    return wide.astype(I16)


def hot16(count, base, value=None):
    one = jnp.ones(base.shape, BF16) if value is None else value
    zero = jnp.zeros(base.shape, BF16)
    tiles = [jnp.where(base == jnp.int16(16 * t), one, zero) for t in range(count // 16)]
    return jnp.concatenate(tiles, axis=0)


def value16(row):
    return jnp.broadcast_to(row, (16, row.shape[1])).astype(BF16)


def pick(wide, mask):
    return jnp.sum(jnp.where(mask, wide, 0.0), axis=0, keepdims=True)


def encode(values):
    largest = jnp.max(jnp.abs(values), axis=1, keepdims=True)
    exponent = jnp.ceil(jnp.log2(jnp.maximum(largest, 1e-30)))
    fixed = jnp.round(values * (jnp.exp2(-exponent) * FULL)).astype(I32)
    eye = iota((LANES, LANES), 0) == iota((LANES, LANES), 1)
    across = [
        jnp.sum(jnp.where(eye, exponent[at : at + LANES], 0.0), axis=0, keepdims=True)
        for at in range(0, values.shape[0], LANES)
    ]
    return fixed, across


def scales_down(across, count, first):
    shape = (count, LANES)
    mask = iota(shape, 1) == iota(shape, 0) + first
    column = jnp.sum(jnp.where(mask, across, 0.0), axis=1, keepdims=True)
    return jnp.exp2(column) * (1.0 / FULL)


def prepare(keys, heavy, key_slot, seg_out, heavy_out, meta_out, slots, hist, meta):
    me = lax.axis_index("gx")
    hk = heavy[...]
    order = iota((1, hk.shape[1]), 1) & 1
    low = hot16(256, spread16(hk & 255), value16((order + 1).astype(F32)))
    flags = dot(low, hot16(512, spread16(hk >> 8)), NT)
    even = key_slot[pl.ds(0, 512, stride=2), :]
    odd = key_slot[pl.ds(1, 512, stride=2), :]

    def turned(part):
        return jnp.concatenate([part(even).astype(F32).T, part(odd).astype(F32).T], axis=0)

    first = jnp.where(flags > 0.0, -flags, turned(lambda s: s & 255))
    second = turned(lambda s: (s >> 8) - 256)
    table = jnp.concatenate([first, second], axis=0).astype(BF16)
    hist[...] = jnp.zeros(hist.shape, F32)
    low_index = iota((256, BLOCK), 0)

    @pl.loop(0, ROWS // BLOCK)
    def _(b):
        span = pl.ds(pl.multiple_of(b * BLOCK, BLOCK), BLOCK)
        key = keys[:, span]
        wide = dot(table, hot16(512, spread16(key >> 8)))
        mask = low_index == (key & 255)
        part = pick(wide[:256], mask).astype(I32)
        slot = (pick(wide[256:], mask).astype(I32) + 256) * 256 + part
        is_heavy = part < 0
        slot = jnp.where(is_heavy, -1, slot)
        slots[:, span] = slot
        spot = (((key >> 9) * HPD - 1 - part) - me * HPM) & (GX * HPM - 1)
        heavy_out[:, span] = jnp.where(is_heavy, spot, -1)
        hist[...] += dot(hot16(512, spread16(slot >> 8)), hot16(256, spread16(slot & 255)), NT)

    present = hist[...] > 0.0
    flag = onehot(present)
    inside = dot(flag, onehot(iota((256, 256), 0) < iota((256, 256), 1)))
    whole = dot(flag, jnp.ones((256, LANES), BF16))
    row, col = iota((512, 512), 0), iota((512, 512), 1)
    before = dot(onehot((col < row) & (col >> 3 == row >> 3)), whole.astype(BF16))
    rank = inside + jnp.concatenate([before, before], axis=1)
    ranks = jnp.where(present, rank, 0.0).T.astype(BF16)
    meta[...] = jnp.zeros(meta.shape, F32)

    @pl.loop(0, ROWS // BLOCK)
    def _(b):
        span = pl.ds(pl.multiple_of(b * BLOCK, BLOCK), BLOCK)
        slot = slots[:, span]
        heavy_spot = heavy_out[:, span]
        light = slot >= 0
        wide = dot(ranks, hot16(512, spread16(slot >> 8)))
        place = pick(wide, low_index == (slot & 255)).astype(I32)
        seg = (((slot >> 11) - me) & (GX - 1)) * CAPK + place
        seg = jnp.where(light, seg, -1)
        seg_out[:, span] = seg
        base = spread16(jnp.where(light, place, -1))
        kinds = jnp.concatenate(
            [
                hot16(64, base),
                hot16(64, base, value16((slot & 255).astype(F32))),
                hot16(64, base, value16(((slot >> 8) & 7).astype(F32))),
                hot16(64, spread16(jnp.where(light, -1, heavy_spot & (HPM - 1)))),
            ],
            axis=0,
        )
        step = jnp.where(light, seg >> 6, heavy_spot >> 3)
        meta[...] += dot(kinds, hot16(LANES, spread16(step)), NT)

    turn = meta[...].T
    left = iota((GX, LANES), 1) < 64

    def doubled(pair):
        swapped = pltpu.roll(pair, 64, 1)
        return jnp.where(left, pair, swapped), jnp.where(left, swapped, pair)

    count, low_sum = doubled(turn[:GX, :LANES])
    high_sum, heavies = doubled(turn[:GX, LANES:])
    share = 1.0 / jnp.maximum(count, 1.0)
    low_slot = jnp.floor(low_sum * share + 0.5)
    high_slot = jnp.floor(high_sum * share + 0.5)
    slot = jnp.where(count > 0.0, high_slot * 256.0 + low_slot, -1.0)
    blank = jnp.zeros((GX, LANES), F32)
    for k, rows in enumerate([count, slot, heavies] + [blank] * 5):
        meta_out[:, k, :] = rows.astype(I32)


def owner_table(me, key_slot, local, rank, spread, sp):
    mine_slot = key_slot[...] - me * OWN
    mine = (mine_slot >= 0) & (mine_slot < OWN)
    flag = onehot(mine)
    inside = dot(flag, onehot(iota((LANES, LANES), 0) < iota((LANES, LANES), 1)))
    whole = dot(flag, jnp.ones((LANES, LANES), BF16))
    line = iota(whole.shape, 0) & 3
    for t in range(1, 4):
        inside = inside + jnp.where(line >= t, pltpu.roll(whole, t, 0), 0.0)
    rank[...] = jnp.where(mine, inside, -1.0)
    local[...] = mine_slot.astype(F32)
    eight = iota((KPP, LANES), 0).astype(F32)

    @pl.loop(0, GX)
    def _(x):
        at = pl.ds(pl.multiple_of(x * 16, 16), 16)
        ranks, locals_ = rank[at, :], local[at, :]
        for y in range(GY):
            acc = jnp.zeros((KPP, LANES), F32)
            for j in range(4):
                n = y * 4 + j
                acc = acc + jnp.where(eight == ranks[n : n + 1], locals_[n : n + 1], 0.0)
            spread[pl.ds(pl.multiple_of(y * KEY_DEV + x * KPP, KPP), KPP), :] = acc

    slot = jnp.sum(spread[...], axis=1, keepdims=True)
    sp[...] = jnp.broadcast_to(slot, spread.shape).astype(I32).astype(I16)


def join_table(me_x, me_y, key_slot, perm):
    first = (me_x * GY + me_y) * 4
    owner = (key_slot[pl.ds(first, 4), :] >> 11).astype(F32)
    across = jnp.concatenate([owner[j : j + 1] for j in range(4)], axis=1)
    down = jnp.concatenate([owner, owner], axis=0).T
    index = iota((LANES, KEY_DEV), 1)
    for j in range(4):
        column = down[:, j : j + 1]
        earlier = index < iota((LANES, KEY_DEV), 0) + j * LANES
        same = jnp.where((column == across) & earlier, 1.0, 0.0)
        rank = jnp.sum(same, axis=1, keepdims=True).astype(I32)
        step = (me_x - column.astype(I32)) & (GX - 1)
        perm[j * LANES : (j + 1) * LANES, :] = onehot(step * KPP + rank == index)


def fused(
    heavy, seg, heavy_seg, meta, measures, key_slot, orders,
    result, report, slot_rows,
    send, got, side, acc, sp, spread, local, rank, perm,
    out2, in2, out3, in3, totals, hist, heavies, tallies,
    s_main, r_main, s_two, r_two, s_three, r_three,
):
    me_x, me_y = lax.axis_index("gx"), lax.axis_index("gy")
    barrier = pltpu.get_barrier_semaphore()

    def along_x(s):
        return (lax.rem(me_x + s, GX), me_y)

    def along_y(s):
        return (me_x, lax.rem(me_y + s, GY))

    def copy(src, dst, send_sem, recv_sem, s, target):
        return pltpu.make_async_remote_copy(
            src_ref=src, dst_ref=dst, send_sem=send_sem.at[s], recv_sem=recv_sem.at[s],
            device_id=target, device_id_type=MESH,
        )

    def main_copy(s):
        return copy(send.at[s], got.at[s], s_main, r_main, s, along_x(s))

    def two_copy(s):
        return copy(out2.at[s], in2.at[s], s_two, r_two, s, along_y(s))

    def three_copy(s):
        x = lax.rem(me_x + s, GX)
        return copy(out3.at[x], in3.at[s], s_three, r_three, s, (x, me_y))

    @pl.loop(1, GX)
    def _(s):
        pl.semaphore_signal(barrier, inc=1, device_id=along_x(s), device_id_type=MESH)

    for s in range(1, GY):
        pl.semaphore_signal(barrier, inc=1, device_id=along_y(s), device_id_type=MESH)

    def segment_sums(row, base):
        total = jnp.zeros((CHUNK, LANES), F32)
        for b in range(ROWS // BLOCK):
            span = slice(b * BLOCK, (b + 1) * BLOCK)
            hot = hot16(CHUNK, spread16(row[:, span] - base))
            total = total + dot(hot, measures[span, :])
        return total

    fixed, exponents = encode(segment_sums(heavy_seg, 0))
    last = iota((8, LANES), 0) == 7
    for s in range(GX):
        side[s, 0:HPM] = fixed[s * HPM : (s + 1) * HPM]
        side[s, HPM:SIDE] = jnp.where(last, exponents[s // 16].astype(I32), meta[s])

    left = iota((1, LANES), 1) < CAPK
    scale_line = iota((SIDE, LANES), 0) == SIDE - 2
    pl.semaphore_wait(barrier, GX - 1 + GY - 1)

    @pl.loop(0, CHUNKS)
    def _(c):
        fixed, exponents = encode(segment_sums(seg, c * CHUNK))
        for i in range(STEPS):
            s = c * STEPS + i
            pair = exponents[i // 2].astype(I32)
            swapped = pltpu.roll(pair, CAPK, 1)
            both = jnp.where(left, swapped, pair) if i % 2 else jnp.where(left, pair, swapped)
            send[s, 0:CAPK] = fixed[i * CAPK : (i + 1) * CAPK].astype(I16)
            send[s, CAPK:MESSAGE] = jnp.where(scale_line, both, side[s]).astype(I16)

        @pl.when(c == 0)
        def _():
            got[0] = send[0]

        @pl.when(c > 0)
        def _():
            @pl.loop(jnp.maximum((c - 1) * STEPS, 1), c * STEPS)
            def _(s):
                main_copy(s).start()

    owner_table(me_x, key_slot, local, rank, spread, sp)

    @pl.loop((CHUNKS - 1) * STEPS, GX)
    def _(s):
        main_copy(s).start()

    join_table(me_x, me_y, key_slot, perm)
    acc[...] = jnp.zeros(acc.shape, F32)
    hist[...] = jnp.zeros(hist.shape, F32)
    heavies[...] = jnp.zeros(heavies.shape, F32)
    tallies[...] = jnp.zeros(tallies.shape, F32)

    @pl.loop(0, CHUNKS)
    def _(g):
        @pl.loop(jnp.maximum(g * STEPS, 1), (g + 1) * STEPS)
        def _(s):
            main_copy(s).wait_recv()

        hots, slots, counts = [], [], []
        heavy_sum, heavy_tally = heavies[...], tallies[0:1, :]
        for j in range(STEPS // 2):
            blocks = []
            for i in range(2):
                s = g * STEPS + 2 * j + i
                block = got[s, CAPK:MESSAGE].astype(I32)
                exponents = block[SIDE - 1 : SIDE].astype(F32)
                scale = scales_down(exponents, HPM, (s & 15) * HPM)
                heavy_sum = heavy_sum + block[:HPM].astype(F32) * scale
                heavy_tally = heavy_tally + block[HPM + 2 : HPM + 3].astype(F32)
                blocks.append(block[HPM:])
            rows = jnp.where(left, blocks[0], blocks[1])
            slot = rows[1:2]
            slots.append(slot)
            counts.append(rows[0:1].astype(F32))
            target = jnp.broadcast_to(slot, (16, LANES)).astype(I16)
            one = value16(jnp.exp2(rows[6:7].astype(F32)))
            zero = jnp.zeros((16, LANES), BF16)
            hots.append(
                jnp.concatenate(
                    [
                        jnp.where(sp[16 * t : 16 * t + 16, :] == target, one, zero)
                        for t in range(OWN // 16)
                    ],
                    axis=0,
                )
            )
        heavies[...] = heavy_sum
        tallies[0:1, :] = heavy_tally
        rows = got[pl.ds(g * STEPS, STEPS), 0:CAPK].reshape(CHUNK, LANES).astype(I32)
        pieces = [(rows >> 8).astype(F32).astype(BF16), (rows & 255).astype(F32).astype(BF16)]
        found = dot(jnp.concatenate(hots, axis=1), jnp.concatenate(pieces, axis=1))
        acc[...] += found[:, :LANES] * (256.0 / FULL) + found[:, LANES:] * (1.0 / FULL)
        slot = jnp.concatenate(slots, axis=1)
        count = value16(jnp.concatenate(counts, axis=1))
        hist[...] += dot(
            hot16(16, spread16(slot >> 7)), hot16(LANES, spread16(slot & 127), count), NT
        )

    tally = tallies[0:1, :]
    tally_high = jnp.floor(tally * (1.0 / 16384.0))
    tally_low = tally - tally_high * 16384.0
    heavy_fixed, heavy_exponents = encode(
        jnp.concatenate([heavies[...], jnp.zeros((LANES - HPM, LANES), F32)], axis=0)
    )
    spread[0:HPM, :] = heavy_fixed[:HPM].astype(F32)
    for s in range(1, GY):
        q = lax.rem(me_y + s, GY)
        fixed, exponents = encode(acc[pl.ds(pl.multiple_of(q * KEY_DEV, KEY_DEV), KEY_DEV), :])
        extra = jnp.concatenate(
            [
                hist[pl.ds(q * 4, 4), :],
                *exponents,
                spread[pl.ds(q * HPD, HPD), :],
                heavy_exponents[0], tally_low, tally_high,
                jnp.zeros((3, LANES), F32),
            ],
            axis=0,
        )
        out2[s, KEY_DEV : KEY_DEV + EXTRA] = extra.astype(I32).astype(I16)
        out2[s, 0:KEY_DEV] = fixed.astype(I16)
        if s > 1:
            two_copy(s - 1).start()
    mine = acc[pl.ds(pl.multiple_of(me_y * KEY_DEV, KEY_DEV), KEY_DEV), :]
    slot = sp[pl.ds(pl.multiple_of(me_y * KEY_DEV, KEY_DEV), KEY_DEV), :].astype(I32)
    slot = slot - me_y * KEY_DEV
    totals[...] = mine
    two_copy(GY - 1).start()

    @pl.loop(1, GX)
    def _(s):
        main_copy(s).wait_send()

    slot_total = hist[pl.ds(me_y * 4, 4), :]
    heavy_total = heavies[pl.ds(me_y * HPD, HPD), :]
    for s in range(1, GY):
        two_copy(s).wait_recv()
        part = in2[s, KEY_DEV : KEY_DEV + EXTRA].astype(I32).astype(F32)
        slot_total = slot_total + part[0:4]
        heavy_total = heavy_total + part[8:10] * scales_down(part[10:11], HPD, me_y * HPD)
        tally = tally + part[11:12] + 16384.0 * part[12:13]
        for j in range(4):
            at = slice(j * LANES, (j + 1) * LANES)
            scale = scales_down(part[4 + j : 5 + j], LANES, 0)
            totals[at, :] += in2[s, at].astype(I32).astype(F32) * scale
    slot_rows[...] = slot_total
    wide = jnp.zeros((KEY_DEV, LANES), F32)
    for r in range(4):
        wide = wide + jnp.where(slot >> 7 == r, slot_total[r : r + 1], 0.0)
    wide = jnp.where((slot & 127) == iota((KEY_DEV, LANES), 1), wide, 0.0)
    count = jnp.sum(wide, axis=1, keepdims=True)
    totals[...] = totals[...] * lax.rsqrt(1.0 + count)
    for x in range(GX):
        out3[x] = totals[x * KPP : (x + 1) * KPP, :]
    device = me_x * GY + me_y
    lane = iota((1, LANES), 1)
    sized = []
    for h in range(HPD):
        number = jnp.sum(jnp.where(lane == me_y * HPD + h, tally, 0.0), axis=1, keepdims=True)
        sized.append(heavy_total[h : h + 1] * lax.rsqrt(1.0 + number))
    in3[0] = totals[pl.ds(pl.multiple_of(me_x * KPP, KPP), KPP), :]

    @pl.loop(1, GX)
    def _(s):
        three_copy(s).start()

    line = iota((KEY_DEV, LANES), 0)
    attributes = orders[...].astype(F32)
    heavy_part = jnp.zeros((KEY_DEV, LANES), F32)
    lines = []
    for h in range(HPD):
        spot = heavy[device * HPD + h] - device * KEY_DEV
        here = line == spot
        heavy_part = heavy_part + jnp.where(here, sized[h], 0.0)
        lines.append(jnp.sum(jnp.where(here, attributes, 0.0), axis=0, keepdims=True) * sized[h])
    report[...] = jnp.concatenate(lines, axis=0).astype(BF16)
    for s in range(1, GY):
        two_copy(s).wait_send()

    @pl.loop(1, GX)
    def _(s):
        three_copy(s).wait_recv()

    rows = in3[...].reshape(KEY_DEV, LANES)
    high = rows.astype(BF16)
    low = (rows - high.astype(F32)).astype(BF16)
    both = dot(perm[...], jnp.concatenate([high, low], axis=1))
    found = both[:, :LANES] + both[:, LANES:] + heavy_part
    result[...] = (attributes * found).astype(BF16)

    @pl.loop(1, GX)
    def _(s):
        three_copy(s).wait_send()


def shaped(*dims, dtype=F32):
    return jax.ShapeDtypeStruct(dims, dtype)


def body(measures, row_keys, orders, heavy_keys, key_slot):
    table = key_slot.reshape(key_slot.shape[0] // LANES, LANES)
    seg, heavy_seg, meta = pl.pallas_call(
        prepare,
        out_shape=(
            shaped(1, ROWS, dtype=I32),
            shaped(1, ROWS, dtype=I32),
            shaped(GX, 8, LANES, dtype=I32),
        ),
        in_specs=[VMEM] * 3,
        out_specs=(VMEM,) * 3,
        scratch_shapes=[
            pltpu.VMEM((1, ROWS), I32),
            pltpu.VMEM((512, 256), F32),
            pltpu.VMEM((256, LANES), F32),
        ],
        compiler_params=pltpu.CompilerParams(vmem_limit_bytes=LIMIT),
    )(row_keys.reshape(1, ROWS), heavy_keys.reshape(1, -1), table)
    dma = pltpu.SemaphoreType.DMA
    result, report, slot_rows = pl.pallas_call(
        fused,
        out_shape=(
            shaped(KEY_DEV, LANES, dtype=BF16),
            shaped(HPD, LANES, dtype=BF16),
            shaped(KEY_DEV // LANES, LANES),
        ),
        in_specs=[SMEM] + [VMEM] * 6,
        out_specs=(VMEM,) * 3,
        scratch_shapes=[
            pltpu.VMEM((GX, MESSAGE, LANES), I16),
            pltpu.VMEM((GX, MESSAGE, LANES), I16),
            pltpu.VMEM((GX, SIDE, LANES), I32),
            pltpu.VMEM((OWN, LANES), F32),
            pltpu.VMEM((OWN, LANES), I16),
            pltpu.VMEM((OWN, LANES), F32),
            pltpu.VMEM((1024, LANES), F32),
            pltpu.VMEM((1024, LANES), F32),
            pltpu.VMEM((KEY_DEV, KEY_DEV), BF16),
            pltpu.VMEM((GY, KEY_DEV + EXTRA, LANES), I16),
            pltpu.VMEM((GY, KEY_DEV + EXTRA, LANES), I16),
            pltpu.VMEM((GX, KPP, LANES), F32),
            pltpu.VMEM((GX, KPP, LANES), F32),
            pltpu.VMEM((KEY_DEV, LANES), F32),
            pltpu.VMEM((16, LANES), F32),
            pltpu.VMEM((HPM, LANES), F32),
            pltpu.VMEM((8, LANES), F32),
        ]
        + [dma((GX,))] * 2
        + [dma((GY,))] * 2
        + [dma((GX,))] * 2,
        compiler_params=pltpu.CompilerParams(
            collective_id=0, has_side_effects=True, vmem_limit_bytes=LIMIT
        ),
    )(heavy_keys, seg, heavy_seg, meta, measures, table, orders)
    return (result, report, slot_rows.reshape(KEY_DEV))


def solution(mesh):
    return jax.shard_map(
        body,
        mesh=mesh,
        in_specs=(P(("gx", "gy"), None), P(("gx", "gy")), P(("gx", "gy"), None), P(), P()),
        out_specs=(P(("gx", "gy"), None), P(("gx", "gy"), None), P(("gx", "gy"))),
        check_vma=False,
    )
```

```python
import functools

import jax
import jax.numpy as jnp
from jax import lax
from jax.experimental import pallas as pl
from jax.experimental.pallas import tpu as pltpu
from jax.sharding import PartitionSpec as P

MESH = pl.DeviceIdType.MESH
LANES = 128
F32 = jnp.float32
BF16 = jnp.bfloat16
I32 = jnp.int32
I16 = jnp.int16
VMEM = pl.BlockSpec(memory_space=pltpu.VMEM)
SMEM = pl.BlockSpec(memory_space=pltpu.SMEM)
ANY = pl.BlockSpec(memory_space=pl.ANY)
LIMIT = 60 * 1024 * 1024
NN = (((1,), (0,)), ((), ()))
NT = (((1,), (1,)), ((), ()))

GX, GY = 64, 4
MEMBERS, GROUPS = 64, 4
ROWS = 8192
BLOCK = 2048
CAPK = 64
OWN = 2048
OWN_ROWS = OWN // 128
KEY_DEV = 512
KPP = 8
HPD = 2
HPG = HPD * MEMBERS
STEPS = 8
HALF = CAPK // 2
CHUNK = STEPS * HALF
CHUNKS = MEMBERS // STEPS
EXTRA = 32
FULL = 32000.0


def dot(a, b, dims=NN):
    return lax.dot_general(a, b, dims, preferred_element_type=F32)


def iota(shape, dim):
    return lax.broadcasted_iota(I32, shape, dim)


def onehot(mask):
    return jnp.where(mask, 1.0, 0.0).astype(BF16)


def spread16(row):
    wide = jnp.broadcast_to(row, (16, row.shape[1])) - iota((16, row.shape[1]), 0)
    return wide.astype(I16)


def hot16(count, base, value=None):
    one = jnp.ones(base.shape, BF16) if value is None else value
    zero = jnp.zeros(base.shape, BF16)
    tiles = [jnp.where(base == jnp.int16(16 * t), one, zero) for t in range(count // 16)]
    return jnp.concatenate(tiles, axis=0)


def value16(row):
    return jnp.broadcast_to(row, (16, row.shape[1])).astype(BF16)


def pick(wide, mask):
    return jnp.sum(jnp.where(mask, wide, 0.0), axis=0, keepdims=True)


def power_of(values):
    largest = jnp.max(jnp.abs(values), axis=1, keepdims=True)
    exponent = jnp.ceil(jnp.log2(jnp.maximum(largest, 1e-30)))
    return jnp.round(values * (jnp.exp2(-exponent) * FULL)).astype(I32), exponent


def encode(values):
    fixed, exponent = power_of(values)
    eye = iota((LANES, LANES), 0) == iota((LANES, LANES), 1)
    across = [
        jnp.sum(jnp.where(eye, exponent[at : at + LANES], 0.0), axis=0, keepdims=True)
        for at in range(0, values.shape[0], LANES)
    ]
    return fixed, across


def scales_down(across, count, first):
    shape = (count, LANES)
    mask = iota(shape, 1) == iota(shape, 0) + first
    column = jnp.sum(jnp.where(mask, across, 0.0), axis=1, keepdims=True)
    return jnp.exp2(column) * (1.0 / FULL)


def member_of(block):
    member = (block >> 6) * 16 + (block & 3) * 4 + ((block >> 3) & 1) * 2 + ((block >> 2) & 1)
    return member, (block >> 4) & 3


def find_slots(keys, heavy, key_slot, slots, heavy_spot, hist, heavy_hist):
    hk = heavy[...]
    order = iota((1, hk.shape[1]), 1) & 1
    low = hot16(256, spread16(hk & 255), value16((order + 1).astype(F32)))
    flags = dot(low, hot16(512, spread16(hk >> 8)), NT)
    even = key_slot[pl.ds(0, 512, stride=2), :]
    odd = key_slot[pl.ds(1, 512, stride=2), :]

    def turned(part):
        return jnp.concatenate([part(even).astype(F32).T, part(odd).astype(F32).T], axis=0)

    first = jnp.where(flags > 0.0, -flags, turned(lambda s: s & 255))
    second = turned(lambda s: (s >> 8) - 256)
    table = jnp.concatenate([first, second], axis=0).astype(BF16)
    hist[...] = jnp.zeros(hist.shape, F32)
    heavy_hist[...] = jnp.zeros(heavy_hist.shape, F32)
    low_index = iota((256, BLOCK), 0)

    @pl.loop(0, ROWS // BLOCK)
    def _(b):
        span = pl.ds(pl.multiple_of(b * BLOCK, BLOCK), BLOCK)
        key = keys[:, span]
        wide = dot(table, hot16(512, spread16(key >> 8)))
        mask = low_index == (key & 255)
        part = pick(wide[:256], mask).astype(I32)
        slot = (pick(wide[256:], mask).astype(I32) + 256) * 256 + part
        is_heavy = part < 0
        slot = jnp.where(is_heavy, -1, slot)
        slots[:, span] = slot
        member, group = member_of(key >> 9)
        spot = jnp.where(is_heavy, group * HPG + member * HPD - 1 - part, -1)
        heavy_spot[:, span] = spot
        hist[...] += dot(hot16(512, spread16(slot >> 8)), hot16(256, spread16(slot & 255)), NT)
        heavy_hist[...] += dot(
            hot16(16, spread16(spot >> 7)), hot16(LANES, spread16(spot & 127)), NT
        )


def find_ranks(me, slots, heavy_spot, seg_out, hist, meta, side, measures, pairs):
    present = hist[...] > 0.0
    flag = onehot(present)
    inside = dot(flag, onehot(iota((256, 256), 0) < iota((256, 256), 1)))
    whole = dot(flag, jnp.ones((256, LANES), BF16))
    row, col = iota((512, 512), 0), iota((512, 512), 1)
    before = dot(onehot((col < row) & (col >> 3 == row >> 3)), whole.astype(BF16))
    rank = inside + jnp.concatenate([before, before], axis=1)
    ranks = jnp.where(present, rank, 0.0).T.astype(BF16)
    meta[...] = jnp.zeros(meta.shape, F32)
    low_index = iota((256, BLOCK), 0)

    @pl.loop(0, ROWS // BLOCK)
    def _(b):
        span = pl.ds(pl.multiple_of(b * BLOCK, BLOCK), BLOCK)
        slot = slots[:, span]
        light = slot >= 0
        wide = dot(ranks, hot16(512, spread16(slot >> 8)))
        place = pick(wide, low_index == (slot & 255)).astype(I32)
        step = ((slot >> 11) - me) & (MEMBERS - 1)
        seg_out[:, span] = jnp.where(light, step * HALF + (place & (HALF - 1)), -1)
        bit = jnp.where(light, place >> 5, heavy_spot[:, span] & 1).astype(F32)
        bits = [bit[:, i * LANES : (i + 1) * LANES] for i in range(BLOCK // LANES)]
        down = jnp.concatenate(bits, axis=0).T
        for i in range(BLOCK // LANES):
            at = pl.ds(pl.multiple_of(b * BLOCK + i * LANES, LANES), LANES)
            rows = measures[at, :]
            upper = rows * jnp.broadcast_to(down[:, i : i + 1], (LANES, LANES)).astype(BF16)
            pairs[at, LANES:] = upper
            pairs[at, :LANES] = rows - upper
        base = spread16(jnp.where(light, place, -1))
        kinds = jnp.concatenate(
            [
                hot16(64, base),
                hot16(64, base, value16((slot & 255).astype(F32))),
                hot16(64, base, value16(((slot >> 8) & 7).astype(F32))),
            ],
            axis=0,
        )
        meta[0:192, :] += dot(kinds, hot16(LANES, spread16(jnp.where(light, step, -1))), NT)

    turn = meta[...].T
    left = iota((MEMBERS, LANES), 1) < CAPK

    def doubled(pair):
        swapped = pltpu.roll(pair, CAPK, 1)
        return jnp.where(left, pair, swapped), jnp.where(left, swapped, pair)

    count, low_sum = doubled(turn[:MEMBERS, :LANES])
    high_sum, unused = doubled(turn[:MEMBERS, LANES:])
    share = 1.0 / jnp.maximum(count, 1.0)
    low_slot = jnp.floor(low_sum * share + 0.5)
    high_slot = jnp.floor(high_sum * share + 0.5)
    slot = jnp.where(count > 0.0, high_slot * 256.0 + low_slot, -1.0)
    side[:, 0, :] = count
    side[:, 1, :] = slot
    side[:, 3, :] = jnp.zeros((MEMBERS, LANES), F32)


def owner_table(me, key_slot, local, rank, spread, sp):
    mine_slot = key_slot[...] - me * OWN
    mine = (mine_slot >= 0) & (mine_slot < OWN)
    flag = onehot(mine)
    inside = dot(flag, onehot(iota((LANES, LANES), 0) < iota((LANES, LANES), 1)))
    whole = dot(flag, jnp.ones((LANES, LANES), BF16))
    line = iota(whole.shape, 0) & 3
    for t in range(1, 4):
        inside = inside + jnp.where(line >= t, pltpu.roll(whole, t, 0), 0.0)
    rank[...] = jnp.where(mine, inside, -1.0)
    local[...] = mine_slot.astype(F32)
    eight = iota((KPP, LANES), 0).astype(F32)

    @pl.loop(0, GX)
    def _(x):
        at = pl.ds(pl.multiple_of(x * 16, 16), 16)
        ranks, locals_ = rank[at, :], local[at, :]
        for y in range(GY):
            acc = jnp.zeros((KPP, LANES), F32)
            for j in range(4):
                n = y * 4 + j
                acc = acc + jnp.where(eight == ranks[n : n + 1], locals_[n : n + 1], 0.0)
            first = ((x >> 2) & 3) * KEY_DEV
            first = first + ((x >> 4) * 16 + y * 4 + ((x >> 1) & 1) * 2 + (x & 1)) * KPP
            spread[pl.ds(pl.multiple_of(first, KPP), KPP), :] = acc

    slot = jnp.sum(spread[...], axis=1, keepdims=True)
    sp[...] = jnp.broadcast_to(slot, spread.shape).astype(I32).astype(I16)


def join_table(device, me, key_slot, perm):
    first = device * 4
    owner = (key_slot[pl.ds(first, 4), :] >> 11).astype(F32)
    across = jnp.concatenate([owner[j : j + 1] for j in range(4)], axis=1)
    down = jnp.concatenate([owner, owner], axis=0).T
    index = iota((LANES, KEY_DEV), 1)
    for j in range(4):
        column = down[:, j : j + 1]
        earlier = index < iota((LANES, KEY_DEV), 0) + j * LANES
        same = jnp.where((column == across) & earlier, 1.0, 0.0)
        rank = jnp.sum(same, axis=1, keepdims=True).astype(I32)
        step = (me - column.astype(I32)) & (MEMBERS - 1)
        perm[j * LANES : (j + 1) * LANES, :] = onehot(step * KPP + rank == index)


def fused(
    heavy, keys, heavy_row, key_slot, measures_hbm, orders_hbm,
    result, report, slot_rows,
    measures, pairs, orders, slots, heavy_spot, seg, ranks_hist, heavy_hist, meta,
    send, got, side, got_side, acc, sp, spread, local, rank, perm,
    out2, in2, out3, in3, totals, hist,
    hv_sums, hv_in, hm_out, hm_in, slot_out, slot_in,
    local_sem, s_main, r_main, s_side, r_side, s_two, r_two, s_three, r_three,
    s_hv, r_hv, s_hm, r_hm, s_slot, r_slot,
):
    me_x, me_y = lax.axis_index("gx"), lax.axis_index("gy")
    device = me_x * GY + me_y
    me, group = member_of(device)
    barrier = pltpu.get_barrier_semaphore()
    fetch = pltpu.make_async_copy(measures_hbm, measures, local_sem.at[0])
    fetch.start()
    fetch_orders = pltpu.make_async_copy(orders_hbm, orders, local_sem.at[1])
    fetch_orders.start()

    def place(member, its_group):
        x, y = member >> 4, (member >> 2) & 3
        return (x * 8 + its_group * 2 + ((member >> 1) & 1)) * 2 + (member & 1), y

    def along(s):
        return lax.rem(me + s, MEMBERS)

    def in_group(s):
        return place(along(s), group)

    def across(s):
        return place(me, lax.rem(group + s, GROUPS))

    opposite = (me, group)
    alone = group == me_y

    def copy(src, dst, send_sem, recv_sem, s, target):
        return pltpu.make_async_remote_copy(
            src_ref=src, dst_ref=dst, send_sem=send_sem.at[s], recv_sem=recv_sem.at[s],
            device_id=target, device_id_type=MESH,
        )

    def main_copy(s):
        return copy(send.at[s], got.at[s], s_main, r_main, s, in_group(s))

    def side_copy(s):
        return copy(side.at[s], got_side.at[s], s_side, r_side, s, in_group(s))

    def heavy_copy(s):
        return copy(hv_sums.at[lax.rem(group + s, GROUPS)], hv_in.at[s], s_hv, r_hv, s, across(s))

    def member_copy(s):
        return copy(hm_out.at[along(s)], hm_in.at[s], s_hm, r_hm, s, in_group(s))

    def two_copy(s):
        return copy(out2.at[s], in2.at[s], s_two, r_two, s, across(s))

    def three_copy(s):
        return copy(out3.at[along(s)], in3.at[s], s_three, r_three, s, in_group(s))

    def slot_copy():
        return copy(slot_out, slot_in, s_slot, r_slot, 0, opposite)

    @pl.loop(1, MEMBERS)
    def _(s):
        pl.semaphore_signal(barrier, inc=1, device_id=in_group(s), device_id_type=MESH)

    for s in range(1, GROUPS):
        pl.semaphore_signal(barrier, inc=1, device_id=across(s), device_id_type=MESH)

    @pl.when(jnp.logical_not(alone))
    def _():
        pl.semaphore_signal(barrier, inc=1, device_id=opposite, device_id_type=MESH)

    def pair_sums(spots):
        total = jnp.zeros((CHUNK, 2 * LANES), F32)
        for b in range(ROWS // BLOCK):
            span = slice(b * BLOCK, (b + 1) * BLOCK)
            total = total + dot(hot16(CHUNK, spread16(spots(span))), pairs[span, :])
        return total

    find_slots(keys, heavy_row, key_slot, slots, heavy_spot, ranks_hist, heavy_hist)
    fetch.wait()
    find_ranks(me, slots, heavy_spot, seg, ranks_hist, meta, side, measures, pairs)

    @pl.when(alone)
    def _():
        pl.semaphore_wait(barrier, MEMBERS - 1 + GROUPS - 1)

    @pl.when(jnp.logical_not(alone))
    def _():
        pl.semaphore_wait(barrier, MEMBERS + GROUPS - 1)

    left = iota((1, LANES), 1) < CAPK
    lane = iota((HALF, LANES), 1) & (CAPK - 1)
    lower_lane = lane == iota((HALF, LANES), 0)
    upper_lane = lane == iota((HALF, LANES), 0) + HALF

    def start_chunk(c):
        @pl.loop(jnp.maximum(c * STEPS, 1), (c + 1) * STEPS)
        def _(s):
            main_copy(s).start()
            side_copy(s).start()

    @pl.loop(0, CHUNKS)
    def _(c):
        total = pair_sums(lambda span: seg[:, span] - c * CHUNK)
        lower, lower_power = power_of(total[:, :LANES])
        upper, upper_power = power_of(total[:, LANES:])
        for i in range(STEPS):
            s = c * STEPS + i
            at = slice(i * HALF, (i + 1) * HALF)
            powers = jnp.where(lower_lane, lower_power[at], 0.0)
            powers = powers + jnp.where(upper_lane, upper_power[at], 0.0)
            send[s, 0:HALF] = lower[at].astype(I16)
            send[s, HALF:CAPK] = upper[at].astype(I16)
            side[s, 2:3] = jnp.exp2(jnp.sum(powers, axis=0, keepdims=True))

        @pl.when(c == 0)
        def _():
            got[0] = send[0]
            got_side[0] = side[0]
            for h in range(HPG * GROUPS // HPD // CHUNK):
                both = pair_sums(
                    lambda span: jnp.where(heavy_spot[:, span] < 0, -1, heavy_spot[:, span] >> 1)
                    - h * CHUNK
                )
                for k in range(CHUNK // MEMBERS):
                    at = slice(k * MEMBERS, (k + 1) * MEMBERS)
                    n = h * (CHUNK // MEMBERS) + k
                    hv_sums[n, 0:MEMBERS] = both[at, :LANES]
                    hv_sums[n, MEMBERS:HPG] = both[at, LANES:]
                    hv_sums[n, HPG : HPG + 8] = jnp.broadcast_to(
                        heavy_hist[n : n + 1, :], (8, LANES)
                    )

        @pl.when(c > 0)
        def _():
            start_chunk(c - 1)

        @pl.when(c == 1)
        def _():
            for s in range(1, GROUPS):
                heavy_copy(s).start()

        @pl.when(c == CHUNKS // 2)
        def _():
            total = hv_sums[group]
            for s in range(1, GROUPS):
                heavy_copy(s).wait_recv()
                total = total + hv_in[s]
            for m in range(MEMBERS):
                rows = [total[h * MEMBERS + m : h * MEMBERS + m + 1] for h in range(HPD)]
                rows.append(total[HPG : HPG + 2])
                hm_out[m] = jnp.concatenate(rows, axis=0)

    owner_table(me, key_slot, local, rank, spread, sp)
    start_chunk(CHUNKS - 1)

    @pl.loop(1, MEMBERS)
    def _(s):
        member_copy(s).start()

    join_table(device, me, key_slot, perm)
    acc[...] = jnp.zeros(acc.shape, F32)
    hist[...] = jnp.zeros(hist.shape, F32)

    @pl.loop(0, CHUNKS)
    def _(g):
        @pl.loop(jnp.maximum(g * STEPS, 1), (g + 1) * STEPS)
        def _(s):
            main_copy(s).wait_recv()
            side_copy(s).wait_recv()

        hots, wanted, counts = [], [], []
        for j in range(STEPS // 2):
            s = g * STEPS + 2 * j
            rows = jnp.where(left, got_side[s], got_side[s + 1])
            slot = rows[1:2].astype(I32)
            wanted.append(slot)
            counts.append(rows[0:1])
            target = jnp.broadcast_to(slot, (16, LANES)).astype(I16)
            one = value16(rows[2:3])
            zero = jnp.zeros((16, LANES), BF16)
            hots.append(
                jnp.concatenate(
                    [
                        jnp.where(sp[16 * t : 16 * t + 16, :] == target, one, zero)
                        for t in range(OWN // 16)
                    ],
                    axis=0,
                )
            )
        rows = got[pl.ds(g * STEPS, STEPS)].reshape(STEPS * CAPK, LANES).astype(I32)
        pieces = [(rows >> 8).astype(F32).astype(BF16), (rows & 255).astype(F32).astype(BF16)]
        found = dot(jnp.concatenate(hots, axis=1), jnp.concatenate(pieces, axis=1))
        acc[...] += found[:, :LANES] * (256.0 / FULL) + found[:, LANES:] * (1.0 / FULL)
        slot = jnp.concatenate(wanted, axis=1)
        count = value16(jnp.concatenate(counts, axis=1))
        hist[...] += dot(
            hot16(OWN_ROWS, spread16(slot >> 7)), hot16(LANES, spread16(slot & 127), count), NT
        )

    def part_of(q):
        return pl.ds(pl.multiple_of(q * KEY_DEV, KEY_DEV), KEY_DEV)

    slot_total = hist[...]
    for s in range(1, GROUPS):
        fixed, exponents = encode(acc[part_of(lax.rem(group + s, GROUPS)), :])
        extra = jnp.concatenate(
            [slot_total, *exponents, jnp.zeros((EXTRA - OWN_ROWS - 4, LANES), F32)], axis=0
        )
        out2[s, KEY_DEV : KEY_DEV + EXTRA] = extra.astype(I32).astype(I16)
        out2[s, 0:KEY_DEV] = fixed.astype(I16)
        if s > 1:
            two_copy(s - 1).start()
    slot = sp[part_of(group), :].astype(I32)
    totals[...] = acc[part_of(group), :]
    two_copy(GROUPS - 1).start()
    hm_in[0] = hm_out[me]

    @pl.loop(1, MEMBERS)
    def _(s):
        main_copy(s).wait_send()
        side_copy(s).wait_send()
        member_copy(s).wait_send()
        member_copy(s).wait_recv()

    heavy_total = jnp.sum(hm_in[...], axis=0)
    for s in range(1, GROUPS):
        two_copy(s).wait_recv()
        part = in2[s, KEY_DEV : KEY_DEV + EXTRA].astype(I32).astype(F32)
        slot_total = slot_total + part[0:OWN_ROWS]
        for j in range(4):
            at = slice(j * LANES, (j + 1) * LANES)
            scale = scales_down(part[OWN_ROWS + j : OWN_ROWS + 1 + j], LANES, 0)
            totals[at, :] += in2[s, at].astype(I32).astype(F32) * scale
    hist[...] = slot_total
    slot_out[...] = hist[pl.ds(group * 4, 4), :]
    wide = jnp.zeros((KEY_DEV, LANES), F32)
    for r in range(OWN_ROWS):
        wide = wide + jnp.where(slot >> 7 == r, slot_total[r : r + 1], 0.0)
    wide = jnp.where((slot & 127) == iota((KEY_DEV, LANES), 1), wide, 0.0)
    count = jnp.sum(wide, axis=1, keepdims=True)
    totals[...] = totals[...] * lax.rsqrt(1.0 + count)
    for m in range(MEMBERS):
        out3[m] = totals[m * KPP : (m + 1) * KPP, :]
    in3[0] = totals[pl.ds(pl.multiple_of(me * KPP, KPP), KPP), :]
    lane = iota((1, LANES), 1)
    sized = []
    for h in range(HPD):
        number = jnp.sum(
            jnp.where(lane == me * HPD + h, heavy_total[HPD : HPD + 1], 0.0),
            axis=1, keepdims=True,
        )
        sized.append(heavy_total[h : h + 1] * lax.rsqrt(1.0 + number))

    @pl.loop(1, MEMBERS)
    def _(s):
        three_copy(s).start()

    @pl.when(alone)
    def _():
        slot_rows[...] = slot_out[...]

    @pl.when(jnp.logical_not(alone))
    def _():
        slot_copy().start()

    line = iota((KEY_DEV, LANES), 0)
    fetch_orders.wait()
    attributes = orders[...].astype(F32)
    heavy_part = jnp.zeros((KEY_DEV, LANES), F32)
    lines = []
    for h in range(HPD):
        spot = heavy[device * HPD + h] - device * KEY_DEV
        here = line == spot
        heavy_part = heavy_part + jnp.where(here, sized[h], 0.0)
        lines.append(jnp.sum(jnp.where(here, attributes, 0.0), axis=0, keepdims=True) * sized[h])
    report[...] = jnp.concatenate(lines, axis=0).astype(BF16)
    totals[...] = heavy_part
    for s in range(1, GROUPS):
        two_copy(s).wait_send()
        heavy_copy(s).wait_send()

    @pl.when(jnp.logical_not(alone))
    def _():
        slot_copy().wait_send()
        slot_copy().wait_recv()
        slot_rows[...] = slot_in[...]

    @pl.loop(1, MEMBERS)
    def _(s):
        three_copy(s).wait_recv()

    rows = in3[...].reshape(KEY_DEV, LANES)
    high = rows.astype(BF16)
    low = (rows - high.astype(F32)).astype(BF16)
    both = dot(perm[...], jnp.concatenate([high, low], axis=1))
    found = both[:, :LANES] + both[:, LANES:] + totals[...]
    result[...] = (orders[...].astype(F32) * found).astype(BF16)

    @pl.loop(1, MEMBERS)
    def _(s):
        three_copy(s).wait_send()


def hand_on(*refs):
    half = len(refs) // 2
    for source, target in zip(refs[:half], refs[half:]):
        target[...] = source[...]


def shaped(*dims, dtype=F32):
    return jax.ShapeDtypeStruct(dims, dtype)


def body(measures, row_keys, orders, heavy_keys, key_slot):
    table = key_slot.reshape(key_slot.shape[0] // LANES, LANES)
    dma = pltpu.SemaphoreType.DMA
    outs = (
        shaped(KEY_DEV, LANES, dtype=BF16),
        shaped(HPD, LANES, dtype=BF16),
        shaped(KEY_DEV // LANES, LANES),
    )
    found = pl.pallas_call(
        fused,
        out_shape=outs,
        in_specs=[SMEM] + [VMEM] * 3 + [ANY] * 2,
        out_specs=(VMEM,) * 3,
        scratch_shapes=[
            pltpu.VMEM((ROWS, LANES), BF16),
            pltpu.VMEM((ROWS, 2 * LANES), BF16),
            pltpu.VMEM((KEY_DEV, LANES), BF16),
            pltpu.VMEM((1, ROWS), I32),
            pltpu.VMEM((1, ROWS), I32),
            pltpu.VMEM((1, ROWS), I32),
            pltpu.VMEM((512, 256), F32),
            pltpu.VMEM((16, LANES), F32),
            pltpu.VMEM((256, LANES), F32),
            pltpu.VMEM((MEMBERS, CAPK, LANES), I16),
            pltpu.VMEM((MEMBERS, CAPK, LANES), I16),
            pltpu.VMEM((MEMBERS, 4, LANES), F32),
            pltpu.VMEM((MEMBERS, 4, LANES), F32),
            pltpu.VMEM((OWN, LANES), F32),
            pltpu.VMEM((OWN, LANES), I16),
            pltpu.VMEM((OWN, LANES), F32),
            pltpu.VMEM((1024, LANES), F32),
            pltpu.VMEM((1024, LANES), F32),
            pltpu.VMEM((KEY_DEV, KEY_DEV), BF16),
            pltpu.VMEM((GROUPS, KEY_DEV + EXTRA, LANES), I16),
            pltpu.VMEM((GROUPS, KEY_DEV + EXTRA, LANES), I16),
            pltpu.VMEM((MEMBERS, KPP, LANES), F32),
            pltpu.VMEM((MEMBERS, KPP, LANES), F32),
            pltpu.VMEM((KEY_DEV, LANES), F32),
            pltpu.VMEM((OWN_ROWS, LANES), F32),
            pltpu.VMEM((GROUPS, HPG + 8, LANES), F32),
            pltpu.VMEM((GROUPS, HPG + 8, LANES), F32),
            pltpu.VMEM((MEMBERS, 4, LANES), F32),
            pltpu.VMEM((MEMBERS, 4, LANES), F32),
            pltpu.VMEM((4, LANES), F32),
            pltpu.VMEM((4, LANES), F32),
            dma((2,)),
        ]
        + [dma((MEMBERS,))] * 4
        + [dma((GROUPS,))] * 2
        + [dma((MEMBERS,))] * 2
        + [dma((GROUPS,))] * 2
        + [dma((MEMBERS,))] * 2
        + [dma((1,))] * 2,
        compiler_params=pltpu.CompilerParams(
            collective_id=0, has_side_effects=True, vmem_limit_bytes=LIMIT
        ),
    )(heavy_keys, row_keys.reshape(1, ROWS), heavy_keys.reshape(1, -1), table, measures, orders)
    result, report, slot_rows = pl.pallas_call(
        hand_on,
        out_shape=outs,
        in_specs=[VMEM] * 3,
        out_specs=(VMEM,) * 3,
    )(*found)
    return (result, report, slot_rows.reshape(KEY_DEV))


def solution(mesh):
    return jax.shard_map(
        body,
        mesh=mesh,
        in_specs=(P(("gx", "gy"), None), P(("gx", "gy")), P(("gx", "gy"), None), P(), P()),
        out_specs=(P(("gx", "gy"), None), P(("gx", "gy"), None), P(("gx", "gy"))),
        check_vma=False,
    )
```

```python
import functools

import jax
import jax.numpy as jnp
from jax import lax
from jax.experimental import pallas as pl
from jax.experimental.pallas import tpu as pltpu
from jax.sharding import PartitionSpec as P

MESH = pl.DeviceIdType.MESH
LANES = 128
F32 = jnp.float32
BF16 = jnp.bfloat16
I32 = jnp.int32
I16 = jnp.int16
VMEM = pl.BlockSpec(memory_space=pltpu.VMEM)
SMEM = pl.BlockSpec(memory_space=pltpu.SMEM)
ANY = pl.BlockSpec(memory_space=pl.ANY)
LIMIT = 60 * 1024 * 1024
NN = (((1,), (0,)), ((), ()))
NT = (((1,), (1,)), ((), ()))

GX, GY = 64, 4
MEMBERS, GROUPS = 64, 4
ROWS = 8192
BLOCK = 2048
CAPK = 64
OWN = 2048
OWN_ROWS = OWN // 128
KEY_DEV = 512
KPP = 8
HPD = 2
HPG = HPD * MEMBERS
STEPS = 8
TAKEN = 8
HALF = CAPK // 2
CHUNK = STEPS * HALF
CHUNKS = MEMBERS // STEPS
DESCRIBED = 1 if STEPS == 8 else 0
EXTRA = 32
FULL = 32000.0


def dot(a, b, dims=NN):
    return lax.dot_general(a, b, dims, preferred_element_type=F32)


def iota(shape, dim):
    return lax.broadcasted_iota(I32, shape, dim)


def onehot(mask):
    return jnp.where(mask, 1.0, 0.0).astype(BF16)


def spread16(row):
    wide = jnp.broadcast_to(row, (16, row.shape[1])) - iota((16, row.shape[1]), 0)
    return wide.astype(I16)


def hot16(count, base, value=None):
    one = jnp.ones(base.shape, BF16) if value is None else value
    zero = jnp.zeros(base.shape, BF16)
    tiles = [jnp.where(base == jnp.int16(16 * t), one, zero) for t in range(count // 16)]
    return jnp.concatenate(tiles, axis=0)


def value16(row):
    return jnp.broadcast_to(row, (16, row.shape[1])).astype(BF16)


def pick(wide, mask):
    return jnp.sum(jnp.where(mask, wide, 0.0), axis=0, keepdims=True)


def power_of(values):
    largest = jnp.max(jnp.abs(values), axis=1, keepdims=True)
    exponent = jnp.ceil(jnp.log2(jnp.maximum(largest, 1e-30)))
    return jnp.round(values * (jnp.exp2(-exponent) * FULL)).astype(I32), exponent


def encode(values):
    fixed, exponent = power_of(values)
    eye = iota((LANES, LANES), 0) == iota((LANES, LANES), 1)
    across = [
        jnp.sum(jnp.where(eye, exponent[at : at + LANES], 0.0), axis=0, keepdims=True)
        for at in range(0, values.shape[0], LANES)
    ]
    return fixed, across


def scales_down(across, count, first):
    shape = (count, LANES)
    mask = iota(shape, 1) == iota(shape, 0) + first
    column = jnp.sum(jnp.where(mask, across, 0.0), axis=1, keepdims=True)
    return jnp.exp2(column) * (1.0 / FULL)


def member_of(block):
    member = (block >> 6) * 16 + (block & 3) * 4 + ((block >> 3) & 1) * 2 + ((block >> 2) & 1)
    return member, (block >> 4) & 3


def find_slots(keys, heavy, key_slot, slots, heavy_spot, hist, heavy_hist):
    hk = heavy[...]
    order = iota((1, hk.shape[1]), 1) & 1
    low = hot16(256, spread16(hk & 255), value16((order + 1).astype(F32)))
    flags = dot(low, hot16(512, spread16(hk >> 8)), NT)
    even = key_slot[pl.ds(0, 512, stride=2), :]
    odd = key_slot[pl.ds(1, 512, stride=2), :]

    def turned(part):
        return jnp.concatenate([part(even).astype(F32).T, part(odd).astype(F32).T], axis=0)

    first = jnp.where(flags > 0.0, -flags, turned(lambda s: s & 255))
    second = turned(lambda s: (s >> 8) - 256)
    table = jnp.concatenate([first, second], axis=0).astype(BF16)
    hist[...] = jnp.zeros(hist.shape, F32)
    heavy_hist[...] = jnp.zeros(heavy_hist.shape, F32)
    low_index = iota((256, BLOCK), 0)

    @pl.loop(0, ROWS // BLOCK)
    def _(b):
        span = pl.ds(pl.multiple_of(b * BLOCK, BLOCK), BLOCK)
        key = keys[:, span]
        wide = dot(table, hot16(512, spread16(key >> 8)))
        mask = low_index == (key & 255)
        part = pick(wide[:256], mask).astype(I32)
        slot = (pick(wide[256:], mask).astype(I32) + 256) * 256 + part
        is_heavy = part < 0
        slot = jnp.where(is_heavy, -1, slot)
        slots[:, span] = slot
        member, group = member_of(key >> 9)
        spot = jnp.where(is_heavy, group * HPG + member * HPD - 1 - part, -1)
        heavy_spot[:, span] = spot
        hist[...] += dot(hot16(512, spread16(slot >> 8)), hot16(256, spread16(slot & 255)), NT)
        heavy_hist[...] += dot(
            hot16(16, spread16(spot >> 7)), hot16(LANES, spread16(spot & 127)), NT
        )


def find_ranks(me, slots, heavy_spot, seg_out, places, hist, measures, pairs):
    present = hist[...] > 0.0
    flag = onehot(present)
    inside = dot(flag, onehot(iota((256, 256), 0) < iota((256, 256), 1)))
    whole = dot(flag, jnp.ones((256, LANES), BF16))
    row, col = iota((512, 512), 0), iota((512, 512), 1)
    before = dot(onehot((col < row) & (col >> 3 == row >> 3)), whole.astype(BF16))
    rank = inside + jnp.concatenate([before, before], axis=1)
    ranks = jnp.where(present, rank, 0.0).T.astype(BF16)
    low_index = iota((256, BLOCK), 0)

    @pl.loop(0, ROWS // BLOCK)
    def _(b):
        span = pl.ds(pl.multiple_of(b * BLOCK, BLOCK), BLOCK)
        slot = slots[:, span]
        light = slot >= 0
        wide = dot(ranks, hot16(512, spread16(slot >> 8)))
        place = pick(wide, low_index == (slot & 255)).astype(I32)
        places[:, span] = jnp.where(light, place, -1)
        step = ((slot >> 11) - me) & (MEMBERS - 1)
        seg_out[:, span] = jnp.where(light, step * HALF + (place & (HALF - 1)), -1)
        bit = jnp.where(light, place >> 5, heavy_spot[:, span] & 1).astype(F32)
        bits = [bit[:, i * LANES : (i + 1) * LANES] for i in range(BLOCK // LANES)]
        down = jnp.concatenate(bits, axis=0).T
        for i in range(BLOCK // LANES):
            at = pl.ds(pl.multiple_of(b * BLOCK + i * LANES, LANES), LANES)
            rows = measures[at, :]
            upper = rows * jnp.broadcast_to(down[:, i : i + 1], (LANES, LANES)).astype(BF16)
            pairs[at, LANES:] = upper
            pairs[at, :LANES] = rows - upper


def describe(me, slots, places, meta, packed):
    meta[...] = jnp.zeros(meta.shape, F32)

    @pl.loop(0, ROWS // BLOCK)
    def _(b):
        span = pl.ds(pl.multiple_of(b * BLOCK, BLOCK), BLOCK)
        slot = slots[:, span]
        base = spread16(places[:, span])
        kinds = jnp.concatenate(
            [
                hot16(64, base),
                hot16(64, base, value16((slot & 255).astype(F32))),
                hot16(64, base, value16(((slot >> 8) & 7).astype(F32))),
            ],
            axis=0,
        )
        step = jnp.where(slot >= 0, ((slot >> 11) - me) & (MEMBERS - 1), -1)
        meta[0:192, :] += dot(kinds, hot16(LANES, spread16(step)), NT)

    turn = meta[...].T
    count, high_sum = turn[:MEMBERS, :LANES], turn[:MEMBERS, LANES:]
    low_sum = pltpu.roll(count, CAPK, 1)
    share = 1.0 / jnp.maximum(count, 1.0)
    low_slot = jnp.floor(low_sum * share + 0.5)
    high_slot = jnp.floor(high_sum * share + 0.5)
    packed[...] = count * OWN + high_slot * 256.0 + low_slot


def owner_table(me, key_slot, local, rank, spread, sp):
    mine_slot = key_slot[...] - me * OWN
    mine = (mine_slot >= 0) & (mine_slot < OWN)
    flag = onehot(mine)
    inside = dot(flag, onehot(iota((LANES, LANES), 0) < iota((LANES, LANES), 1)))
    whole = dot(flag, jnp.ones((LANES, LANES), BF16))
    line = iota(whole.shape, 0) & 3
    for t in range(1, 4):
        inside = inside + jnp.where(line >= t, pltpu.roll(whole, t, 0), 0.0)
    rank[...] = jnp.where(mine, inside, -1.0)
    local[...] = mine_slot.astype(F32)
    eight = iota((KPP, LANES), 0).astype(F32)

    @pl.loop(0, GX)
    def _(x):
        at = pl.ds(pl.multiple_of(x * 16, 16), 16)
        ranks, locals_ = rank[at, :], local[at, :]
        for y in range(GY):
            acc = jnp.zeros((KPP, LANES), F32)
            for j in range(4):
                n = y * 4 + j
                acc = acc + jnp.where(eight == ranks[n : n + 1], locals_[n : n + 1], 0.0)
            first = ((x >> 2) & 3) * KEY_DEV
            first = first + ((x >> 4) * 16 + y * 4 + ((x >> 1) & 1) * 2 + (x & 1)) * KPP
            spread[pl.ds(pl.multiple_of(first, KPP), KPP), :] = acc

    slot = jnp.sum(spread[...], axis=1, keepdims=True)
    sp[...] = jnp.broadcast_to(slot, spread.shape).astype(I32).astype(I16)


def join_table(device, me, key_slot, perm):
    first = device * 4
    owner = (key_slot[pl.ds(first, 4), :] >> 11).astype(F32)
    across = jnp.concatenate([owner[j : j + 1] for j in range(4)], axis=1)
    down = jnp.concatenate([owner, owner], axis=0).T
    index = iota((LANES, KEY_DEV), 1)
    for j in range(4):
        column = down[:, j : j + 1]
        earlier = index < iota((LANES, KEY_DEV), 0) + j * LANES
        same = jnp.where((column == across) & earlier, 1.0, 0.0)
        rank = jnp.sum(same, axis=1, keepdims=True).astype(I32)
        step = (me - column.astype(I32)) & (MEMBERS - 1)
        perm[j * LANES : (j + 1) * LANES, :] = onehot(step * KPP + rank == index)


def fused(
    heavy, keys, heavy_row, key_slot_hbm, measures_hbm, orders_hbm,
    result, report, slot_rows,
    key_slot, measures, pairs, orders, slots, heavy_spot, seg, places, packed, scales, ranks_hist, heavy_hist, meta,
    send, got, side, got_side, acc, sp, spread, local, rank, perm,
    out2, in2, out3, in3, totals, hist,
    hv_sums, hv_in, hm_out, hm_in, slot_out, slot_in,
    local_sem, s_main, r_main, s_side, r_side, s_two, r_two, s_three, r_three,
    s_hv, r_hv, s_hm, r_hm, s_slot, r_slot,
):
    me_x, me_y = lax.axis_index("gx"), lax.axis_index("gy")
    device = me_x * GY + me_y
    me, group = member_of(device)
    barrier = pltpu.get_barrier_semaphore()
    fetch_slots = pltpu.make_async_copy(key_slot_hbm, key_slot, local_sem.at[2])
    fetch_slots.start()
    fetch = pltpu.make_async_copy(measures_hbm, measures, local_sem.at[0])
    fetch.start()
    fetch_orders = pltpu.make_async_copy(orders_hbm, orders, local_sem.at[1])
    fetch_orders.start()

    def place(member, its_group):
        x, y = member >> 4, (member >> 2) & 3
        return (x * 8 + its_group * 2 + ((member >> 1) & 1)) * 2 + (member & 1), y

    def along(s):
        return lax.rem(me + s, MEMBERS)

    def in_group(s):
        return place(along(s), group)

    def across(s):
        return place(me, lax.rem(group + s, GROUPS))

    opposite = (me, group)
    alone = group == me_y

    def copy(src, dst, send_sem, recv_sem, s, target):
        return pltpu.make_async_remote_copy(
            src_ref=src, dst_ref=dst, send_sem=send_sem.at[s], recv_sem=recv_sem.at[s],
            device_id=target, device_id_type=MESH,
        )

    def main_copy(s):
        return copy(send.at[s], got.at[s], s_main, r_main, s, in_group(s))

    def side_copy(s):
        return copy(side.at[s], got_side.at[s], s_side, r_side, s, in_group(s))

    def heavy_copy(s):
        return copy(hv_sums.at[lax.rem(group + s, GROUPS)], hv_in.at[s], s_hv, r_hv, s, across(s))

    def member_copy(s):
        return copy(hm_out.at[along(s)], hm_in.at[s], s_hm, r_hm, s, in_group(s))

    def two_copy(s):
        return copy(out2.at[s], in2.at[s], s_two, r_two, s, across(s))

    def three_copy(s):
        return copy(out3.at[along(s)], in3.at[s], s_three, r_three, s, in_group(s))

    def slot_copy():
        return copy(slot_out, slot_in, s_slot, r_slot, 0, opposite)

    for s in range(1, MEMBERS):
        pl.semaphore_signal(barrier, inc=1, device_id=in_group(s), device_id_type=MESH)

    for s in range(1, GROUPS):
        pl.semaphore_signal(barrier, inc=1, device_id=across(s), device_id_type=MESH)

    @pl.when(jnp.logical_not(alone))
    def _():
        pl.semaphore_signal(barrier, inc=1, device_id=opposite, device_id_type=MESH)

    def pair_sums(count, spots):
        total = jnp.zeros((count, 2 * LANES), F32)
        for b in range(ROWS // BLOCK):
            span = slice(b * BLOCK, (b + 1) * BLOCK)
            total = total + dot(hot16(count, spread16(spots(span))), pairs[span, :])
        return total

    fetch_slots.wait()
    find_slots(keys, heavy_row, key_slot, slots, heavy_spot, ranks_hist, heavy_hist)
    fetch.wait()
    find_ranks(me, slots, heavy_spot, seg, places, ranks_hist, measures, pairs)

    @pl.when(alone)
    def _():
        pl.semaphore_wait(barrier, MEMBERS - 1 + GROUPS - 1)

    @pl.when(jnp.logical_not(alone))
    def _():
        pl.semaphore_wait(barrier, MEMBERS + GROUPS - 1)

    left = iota((1, LANES), 1) < CAPK
    lane = iota((HALF, LANES), 1) & (CAPK - 1)
    lower_lane = lane == iota((HALF, LANES), 0)
    upper_lane = lane == iota((HALF, LANES), 0) + HALF

    def start_sides(c):
        for i in range(STEPS):
            s = c * STEPS + i
            side[s] = jnp.where(left, packed[pl.ds(s, 1), :], scales[s])

        @pl.loop(jnp.maximum(c * STEPS, 1), (c + 1) * STEPS)
        def _(s):
            side_copy(s).start()

    @pl.loop(0, CHUNKS)
    def _(c):
        total = pair_sums(CHUNK, lambda span: seg[:, span] - c * CHUNK)
        lower, lower_power = power_of(total[:, :LANES])
        upper, upper_power = power_of(total[:, LANES:])
        for i in range(STEPS):
            s = c * STEPS + i
            at = slice(i * HALF, (i + 1) * HALF)
            powers = jnp.where(lower_lane, lower_power[at], 0.0)
            powers = powers + jnp.where(upper_lane, upper_power[at], 0.0)
            send[s, 0:HALF] = lower[at].astype(I16)
            send[s, HALF:CAPK] = upper[at].astype(I16)
            scales[s] = jnp.exp2(jnp.sum(powers, axis=0, keepdims=True))

        @pl.loop(jnp.maximum(c * STEPS, 1), (c + 1) * STEPS)
        def _(s):
            main_copy(s).start()

        @pl.when(c == DESCRIBED)
        def _():
            describe(me, slots, places, meta, packed)
            for n in range(DESCRIBED):
                start_sides(n)
            got[0] = send[0]

        @pl.when(c >= DESCRIBED)
        def _():
            start_sides(c)

        @pl.when(c == DESCRIBED + 1)
        def _():
            both = pair_sums(
                MEMBERS * GROUPS,
                lambda span: jnp.where(heavy_spot[:, span] < 0, -1, heavy_spot[:, span] >> 1),
            )
            for n in range(GROUPS):
                at = slice(n * MEMBERS, (n + 1) * MEMBERS)
                hv_sums[n, 0:MEMBERS] = both[at, :LANES]
                hv_sums[n, MEMBERS:HPG] = both[at, LANES:]
                hv_sums[n, HPG : HPG + 8] = jnp.broadcast_to(heavy_hist[n : n + 1, :], (8, LANES))

        @pl.when(c == DESCRIBED + 2)
        def _():
            for s in range(1, GROUPS):
                heavy_copy(s).start()

    got_side[0] = side[0]
    owner_table(me, key_slot, local, rank, spread, sp)

    total = hv_sums[group]
    for s in range(1, GROUPS):
        heavy_copy(s).wait_recv()
        total = total + hv_in[s]
    for m in range(MEMBERS):
        rows = [total[h * MEMBERS + m : h * MEMBERS + m + 1] for h in range(HPD)]
        rows.append(total[HPG : HPG + 2])
        hm_out[m] = jnp.concatenate(rows, axis=0)
    join_table(device, me, key_slot, perm)

    @pl.loop(1, MEMBERS)
    def _(s):
        member_copy(s).start()

    acc[...] = jnp.zeros(acc.shape, F32)
    hist[...] = jnp.zeros(hist.shape, F32)

    @pl.loop(0, MEMBERS // TAKEN)
    def _(g):
        @pl.loop(jnp.maximum(g * TAKEN, 1), (g + 1) * TAKEN)
        def _(s):
            main_copy(s).wait_recv()
            side_copy(s).wait_recv()

        hots, wanted, counts = [], [], []
        for j in range(TAKEN // 2):
            s = g * TAKEN + 2 * j
            a, b = got_side[s], got_side[s + 1]
            entry = jnp.where(left, a, pltpu.roll(b, CAPK, 1)).astype(I32)
            slot = jnp.where(entry >= OWN, entry & (OWN - 1), -1)
            wanted.append(slot)
            counts.append((entry >> 11).astype(F32))
            target = jnp.broadcast_to(slot, (16, LANES)).astype(I16)
            one = value16(jnp.where(left, pltpu.roll(a, CAPK, 1), b))
            zero = jnp.zeros((16, LANES), BF16)
            hots.append(
                jnp.concatenate(
                    [
                        jnp.where(sp[16 * t : 16 * t + 16, :] == target, one, zero)
                        for t in range(OWN // 16)
                    ],
                    axis=0,
                )
            )
        rows = got[pl.ds(g * TAKEN, TAKEN)].reshape(TAKEN * CAPK, LANES).astype(I32)
        low = rows & 255
        pieces = [(rows - low).astype(F32).astype(BF16), low.astype(F32).astype(BF16)]
        found = dot(jnp.concatenate(hots, axis=1), jnp.concatenate(pieces, axis=1))
        acc[...] += found[:, :LANES] + found[:, LANES:]
        slot = jnp.concatenate(wanted, axis=1)
        count = value16(jnp.concatenate(counts, axis=1))
        hist[...] += dot(
            hot16(OWN_ROWS, spread16(slot >> 7)), hot16(LANES, spread16(slot & 127), count), NT
        )

    def part_of(q):
        return pl.ds(pl.multiple_of(q * KEY_DEV, KEY_DEV), KEY_DEV)

    slot_total = hist[...]
    for s in range(1, GROUPS):
        fixed, exponents = encode(acc[part_of(lax.rem(group + s, GROUPS)), :])
        extra = jnp.concatenate(
            [slot_total, *exponents, jnp.zeros((EXTRA - OWN_ROWS - 4, LANES), F32)], axis=0
        )
        out2[s, KEY_DEV : KEY_DEV + EXTRA] = extra.astype(I32).astype(I16)
        out2[s, 0:KEY_DEV] = fixed.astype(I16)
        if s > 1:
            two_copy(s - 1).start()
    slot = sp[part_of(group), :].astype(I32)
    totals[...] = acc[part_of(group), :]
    two_copy(GROUPS - 1).start()
    hm_in[0] = hm_out[me]

    @pl.loop(1, MEMBERS)
    def _(s):
        main_copy(s).wait_send()
        side_copy(s).wait_send()
        member_copy(s).wait_send()
        member_copy(s).wait_recv()

    heavy_total = jnp.sum(hm_in[...], axis=0)
    for s in range(1, GROUPS):
        two_copy(s).wait_recv()
        part = in2[s, KEY_DEV : KEY_DEV + EXTRA].astype(I32).astype(F32)
        slot_total = slot_total + part[0:OWN_ROWS]
        for j in range(4):
            at = slice(j * LANES, (j + 1) * LANES)
            scale = scales_down(part[OWN_ROWS + j : OWN_ROWS + 1 + j], LANES, 0)
            totals[at, :] += in2[s, at].astype(I32).astype(F32) * scale
    hist[...] = slot_total
    slot_out[...] = hist[pl.ds(group * 4, 4), :]
    wide = jnp.zeros((KEY_DEV, LANES), F32)
    for r in range(OWN_ROWS):
        wide = wide + jnp.where(slot >> 7 == r, slot_total[r : r + 1], 0.0)
    wide = jnp.where((slot & 127) == iota((KEY_DEV, LANES), 1), wide, 0.0)
    count = jnp.sum(wide, axis=1, keepdims=True)
    totals[...] = totals[...] * (lax.rsqrt(1.0 + count) * (1.0 / FULL))
    for m in range(MEMBERS):
        out3[m] = totals[m * KPP : (m + 1) * KPP, :]
    in3[0] = totals[pl.ds(pl.multiple_of(me * KPP, KPP), KPP), :]
    lane = iota((1, LANES), 1)
    sized = []
    for h in range(HPD):
        number = jnp.sum(
            jnp.where(lane == me * HPD + h, heavy_total[HPD : HPD + 1], 0.0),
            axis=1, keepdims=True,
        )
        sized.append(heavy_total[h : h + 1] * lax.rsqrt(1.0 + number))

    for s in range(1, MEMBERS):
        three_copy(s).start()

    @pl.when(alone)
    def _():
        slot_rows[...] = slot_out[...]

    @pl.when(jnp.logical_not(alone))
    def _():
        slot_copy().start()

    line = iota((KEY_DEV, LANES), 0)
    fetch_orders.wait()
    attributes = orders[...].astype(F32)
    heavy_part = jnp.zeros((KEY_DEV, LANES), F32)
    lines = []
    for h in range(HPD):
        spot = heavy[device * HPD + h] - device * KEY_DEV
        here = line == spot
        heavy_part = heavy_part + jnp.where(here, sized[h], 0.0)
        lines.append(jnp.sum(jnp.where(here, attributes, 0.0), axis=0, keepdims=True) * sized[h])
    report[...] = jnp.concatenate(lines, axis=0).astype(BF16)
    totals[...] = heavy_part
    for s in range(1, GROUPS):
        two_copy(s).wait_send()
        heavy_copy(s).wait_send()

    @pl.when(jnp.logical_not(alone))
    def _():
        slot_copy().wait_send()
        slot_copy().wait_recv()
        slot_rows[...] = slot_in[...]

    @pl.loop(1, MEMBERS)
    def _(s):
        three_copy(s).wait_recv()

    rows = in3[...].reshape(KEY_DEV, LANES)
    high = rows.astype(BF16)
    low = (rows - high.astype(F32)).astype(BF16)
    both = dot(perm[...], jnp.concatenate([high, low], axis=1))
    found = both[:, :LANES] + both[:, LANES:] + totals[...]
    result[...] = (orders[...].astype(F32) * found).astype(BF16)

    @pl.loop(1, MEMBERS)
    def _(s):
        three_copy(s).wait_send()


def hand_on(*refs):
    half = len(refs) // 2
    for source, target in zip(refs[:half], refs[half:]):
        target[...] = source[...]


def shaped(*dims, dtype=F32):
    return jax.ShapeDtypeStruct(dims, dtype)


def body(measures, row_keys, orders, heavy_keys, key_slot):
    table = key_slot.reshape(key_slot.shape[0] // LANES, LANES)
    dma = pltpu.SemaphoreType.DMA
    outs = (
        shaped(KEY_DEV, LANES, dtype=BF16),
        shaped(HPD, LANES, dtype=BF16),
        shaped(KEY_DEV // LANES, LANES),
    )
    found = pl.pallas_call(
        fused,
        out_shape=outs,
        in_specs=[SMEM] + [VMEM] * 2 + [ANY] * 3,
        out_specs=(VMEM,) * 3,
        scratch_shapes=[
            pltpu.VMEM((KEY_DEV * MEMBERS * GROUPS // LANES, LANES), I32),
            pltpu.VMEM((ROWS, LANES), BF16),
            pltpu.VMEM((ROWS, 2 * LANES), BF16),
            pltpu.VMEM((KEY_DEV, LANES), BF16),
            pltpu.VMEM((1, ROWS), I32),
            pltpu.VMEM((1, ROWS), I32),
            pltpu.VMEM((1, ROWS), I32),
            pltpu.VMEM((1, ROWS), I32),
            pltpu.VMEM((MEMBERS, LANES), F32),
            pltpu.VMEM((MEMBERS, 1, LANES), F32),
            pltpu.VMEM((512, 256), F32),
            pltpu.VMEM((16, LANES), F32),
            pltpu.VMEM((256, LANES), F32),
            pltpu.VMEM((MEMBERS, CAPK, LANES), I16),
            pltpu.VMEM((MEMBERS, CAPK, LANES), I16),
            pltpu.VMEM((MEMBERS, 1, LANES), F32),
            pltpu.VMEM((MEMBERS, 1, LANES), F32),
            pltpu.VMEM((OWN, LANES), F32),
            pltpu.VMEM((OWN, LANES), I16),
            pltpu.VMEM((OWN, LANES), F32),
            pltpu.VMEM((1024, LANES), F32),
            pltpu.VMEM((1024, LANES), F32),
            pltpu.VMEM((KEY_DEV, KEY_DEV), BF16),
            pltpu.VMEM((GROUPS, KEY_DEV + EXTRA, LANES), I16),
            pltpu.VMEM((GROUPS, KEY_DEV + EXTRA, LANES), I16),
            pltpu.VMEM((MEMBERS, KPP, LANES), F32),
            pltpu.VMEM((MEMBERS, KPP, LANES), F32),
            pltpu.VMEM((KEY_DEV, LANES), F32),
            pltpu.VMEM((OWN_ROWS, LANES), F32),
            pltpu.VMEM((GROUPS, HPG + 8, LANES), F32),
            pltpu.VMEM((GROUPS, HPG + 8, LANES), F32),
            pltpu.VMEM((MEMBERS, 4, LANES), F32),
            pltpu.VMEM((MEMBERS, 4, LANES), F32),
            pltpu.VMEM((4, LANES), F32),
            pltpu.VMEM((4, LANES), F32),
            dma((3,)),
        ]
        + [dma((MEMBERS,))] * 4
        + [dma((GROUPS,))] * 2
        + [dma((MEMBERS,))] * 2
        + [dma((GROUPS,))] * 2
        + [dma((MEMBERS,))] * 2
        + [dma((1,))] * 2,
        compiler_params=pltpu.CompilerParams(
            collective_id=0, has_side_effects=True, vmem_limit_bytes=LIMIT
        ),
    )(heavy_keys, row_keys.reshape(1, ROWS), heavy_keys.reshape(1, -1), table, measures, orders)
    result, report, slot_rows = pl.pallas_call(
        hand_on,
        out_shape=outs,
        in_specs=[VMEM] * 3,
        out_specs=(VMEM,) * 3,
    )(*found)
    return (result, report, slot_rows.reshape(KEY_DEV))


def solution(mesh):
    return jax.shard_map(
        body,
        mesh=mesh,
        in_specs=(P(("gx", "gy"), None), P(("gx", "gy")), P(("gx", "gy"), None), P(), P()),
        out_specs=(P(("gx", "gy"), None), P(("gx", "gy"), None), P(("gx", "gy"))),
        check_vma=False,
    )
```

```python
import functools

import jax
import jax.numpy as jnp
from jax import lax
from jax.experimental import pallas as pl
from jax.experimental.pallas import tpu as pltpu
from jax.sharding import PartitionSpec as P

MESH = pl.DeviceIdType.MESH
LANES = 128
F32 = jnp.float32
BF16 = jnp.bfloat16
I32 = jnp.int32
I16 = jnp.int16
VMEM = pl.BlockSpec(memory_space=pltpu.VMEM)
SMEM = pl.BlockSpec(memory_space=pltpu.SMEM)
ANY = pl.BlockSpec(memory_space=pl.ANY)
LIMIT = 60 * 1024 * 1024
NN = (((1,), (0,)), ((), ()))
NT = (((1,), (1,)), ((), ()))

GX, GY = 64, 4
MEMBERS, GROUPS = 64, 4
ROWS = 8192
BLOCK = 2048
CAPK = 64
OWN = 2048
OWN_ROWS = OWN // 128
KEY_DEV = 512
KPP = 8
HPD = 2
HPG = HPD * MEMBERS
STEPS = 8
TAKEN = 8
HALF = CAPK // 2
CHUNK = STEPS * HALF
CHUNKS = MEMBERS // STEPS
DESCRIBED = 1 if STEPS == 8 else 0
EXTRA = 32
FULL = 32000.0


def hops(s):
    return sum(min(n, 4 - n) for n in (s >> 4, (s >> 2) & 3)) + ((s >> 1) & 1)


FAR_FIRST = sorted(range(1, MEMBERS), key=lambda s: -hops(s))


def dot(a, b, dims=NN):
    return lax.dot_general(a, b, dims, preferred_element_type=F32)


def iota(shape, dim):
    return lax.broadcasted_iota(I32, shape, dim)


def onehot(mask):
    return jnp.where(mask, 1.0, 0.0).astype(BF16)


def spread16(row):
    wide = jnp.broadcast_to(row, (16, row.shape[1])) - iota((16, row.shape[1]), 0)
    return wide.astype(I16)


def hot16(count, base, value=None):
    one = jnp.ones(base.shape, BF16) if value is None else value
    zero = jnp.zeros(base.shape, BF16)
    tiles = [jnp.where(base == jnp.int16(16 * t), one, zero) for t in range(count // 16)]
    return jnp.concatenate(tiles, axis=0)


def value16(row):
    return jnp.broadcast_to(row, (16, row.shape[1])).astype(BF16)


def pick(wide, mask):
    return jnp.sum(jnp.where(mask, wide, 0.0), axis=0, keepdims=True)


def power_of(values):
    largest = jnp.max(jnp.abs(values), axis=1, keepdims=True)
    exponent = jnp.ceil(jnp.log2(jnp.maximum(largest, 1e-30)))
    return jnp.round(values * (jnp.exp2(-exponent) * FULL)).astype(I32), exponent


def encode(values):
    fixed, exponent = power_of(values)
    eye = iota((LANES, LANES), 0) == iota((LANES, LANES), 1)
    across = [
        jnp.sum(jnp.where(eye, exponent[at : at + LANES], 0.0), axis=0, keepdims=True)
        for at in range(0, values.shape[0], LANES)
    ]
    return fixed, across


def scales_down(across, count, first):
    shape = (count, LANES)
    mask = iota(shape, 1) == iota(shape, 0) + first
    column = jnp.sum(jnp.where(mask, across, 0.0), axis=1, keepdims=True)
    return jnp.exp2(column) * (1.0 / FULL)


def member_of(block):
    member = (block >> 6) * 16 + (block & 3) * 4 + ((block >> 3) & 1) * 2 + ((block >> 2) & 1)
    return member, (block >> 4) & 3


def find_slots(keys, heavy, key_slot, slots, heavy_spot, hist, heavy_hist):
    hk = heavy[...]
    order = iota((1, hk.shape[1]), 1) & 1
    low = hot16(256, spread16(hk & 255), value16((order + 1).astype(F32)))
    flags = dot(low, hot16(512, spread16(hk >> 8)), NT)
    even = key_slot[pl.ds(0, 512, stride=2), :]
    odd = key_slot[pl.ds(1, 512, stride=2), :]

    def turned(part):
        return jnp.concatenate([part(even).astype(F32).T, part(odd).astype(F32).T], axis=0)

    first = jnp.where(flags > 0.0, -flags, turned(lambda s: s & 255))
    second = turned(lambda s: (s >> 8) - 256)
    table = jnp.concatenate([first, second], axis=0).astype(BF16)
    hist[...] = jnp.zeros(hist.shape, F32)
    heavy_hist[...] = jnp.zeros(heavy_hist.shape, F32)
    low_index = iota((256, BLOCK), 0)

    @pl.loop(0, ROWS // BLOCK)
    def _(b):
        span = pl.ds(pl.multiple_of(b * BLOCK, BLOCK), BLOCK)
        key = keys[:, span]
        wide = dot(table, hot16(512, spread16(key >> 8)))
        mask = low_index == (key & 255)
        part = pick(wide[:256], mask).astype(I32)
        slot = (pick(wide[256:], mask).astype(I32) + 256) * 256 + part
        is_heavy = part < 0
        slot = jnp.where(is_heavy, -1, slot)
        slots[:, span] = slot
        member, group = member_of(key >> 9)
        spot = jnp.where(is_heavy, group * HPG + member * HPD - 1 - part, -1)
        heavy_spot[:, span] = spot
        hist[...] += dot(hot16(512, spread16(slot >> 8)), hot16(256, spread16(slot & 255)), NT)
        heavy_hist[...] += dot(
            hot16(16, spread16(spot >> 7)), hot16(LANES, spread16(spot & 127)), NT
        )


def find_ranks(me, slots, heavy_spot, seg_out, places, hist, measures, pairs):
    present = hist[...] > 0.0
    flag = onehot(present)
    inside = dot(flag, onehot(iota((256, 256), 0) < iota((256, 256), 1)))
    whole = dot(flag, jnp.ones((256, LANES), BF16))
    row, col = iota((512, 512), 0), iota((512, 512), 1)
    before = dot(onehot((col < row) & (col >> 3 == row >> 3)), whole.astype(BF16))
    rank = inside + jnp.concatenate([before, before], axis=1)
    ranks = jnp.where(present, rank, 0.0).T.astype(BF16)
    low_index = iota((256, BLOCK), 0)

    @pl.loop(0, ROWS // BLOCK, unroll=2)
    def _(b):
        span = pl.ds(pl.multiple_of(b * BLOCK, BLOCK), BLOCK)
        slot = slots[:, span]
        light = slot >= 0
        wide = dot(ranks, hot16(512, spread16(slot >> 8)))
        place = pick(wide, low_index == (slot & 255)).astype(I32)
        places[:, span] = jnp.where(light, place, -1)
        step = ((slot >> 11) - me) & (MEMBERS - 1)
        seg_out[:, span] = jnp.where(light, step * HALF + (place & (HALF - 1)), -1)
        bit = jnp.where(light, place >> 5, heavy_spot[:, span] & 1).astype(F32)
        bits = [bit[:, i * LANES : (i + 1) * LANES] for i in range(BLOCK // LANES)]
        down = jnp.concatenate(bits, axis=0).T
        for i in range(BLOCK // LANES):
            at = pl.ds(pl.multiple_of(b * BLOCK + i * LANES, LANES), LANES)
            rows = measures[at, :]
            upper = rows * jnp.broadcast_to(down[:, i : i + 1], (LANES, LANES)).astype(BF16)
            pairs[at, LANES:] = upper
            pairs[at, :LANES] = rows - upper


def describe(me, slots, places, meta, packed):
    meta[...] = jnp.zeros(meta.shape, F32)

    @pl.loop(0, ROWS // BLOCK, unroll=2)
    def _(b):
        span = pl.ds(pl.multiple_of(b * BLOCK, BLOCK), BLOCK)
        slot = slots[:, span]
        base = spread16(places[:, span])
        kinds = jnp.concatenate(
            [
                hot16(64, base),
                hot16(64, base, value16((slot & 255).astype(F32))),
                hot16(64, base, value16(((slot >> 8) & 7).astype(F32))),
            ],
            axis=0,
        )
        step = jnp.where(slot >= 0, ((slot >> 11) - me) & (MEMBERS - 1), -1)
        meta[0:192, :] += dot(kinds, hot16(LANES, spread16(step)), NT)

    turn = meta[...].T
    count, high_sum = turn[:MEMBERS, :LANES], turn[:MEMBERS, LANES:]
    low_sum = pltpu.roll(count, CAPK, 1)
    share = 1.0 / jnp.maximum(count, 1.0)
    low_slot = jnp.floor(low_sum * share + 0.5)
    high_slot = jnp.floor(high_sum * share + 0.5)
    packed[...] = count * OWN + high_slot * 256.0 + low_slot


def owner_table(me, key_slot, local, rank, spread, sp):
    mine_slot = key_slot[...] - me * OWN
    mine = (mine_slot >= 0) & (mine_slot < OWN)
    flag = onehot(mine)
    inside = dot(flag, onehot(iota((LANES, LANES), 0) < iota((LANES, LANES), 1)))
    whole = dot(flag, jnp.ones((LANES, LANES), BF16))
    line = iota(whole.shape, 0) & 3
    for t in range(1, 4):
        inside = inside + jnp.where(line >= t, pltpu.roll(whole, t, 0), 0.0)
    rank[...] = jnp.where(mine, inside, -1.0)
    local[...] = mine_slot.astype(F32)
    eight = iota((KPP, LANES), 0).astype(F32)

    @pl.loop(0, GX)
    def _(x):
        at = pl.ds(pl.multiple_of(x * 16, 16), 16)
        ranks, locals_ = rank[at, :], local[at, :]
        for y in range(GY):
            acc = jnp.zeros((KPP, LANES), F32)
            for j in range(4):
                n = y * 4 + j
                acc = acc + jnp.where(eight == ranks[n : n + 1], locals_[n : n + 1], 0.0)
            first = ((x >> 2) & 3) * KEY_DEV
            first = first + ((x >> 4) * 16 + y * 4 + ((x >> 1) & 1) * 2 + (x & 1)) * KPP
            spread[pl.ds(pl.multiple_of(first, KPP), KPP), :] = acc

    slot = jnp.sum(spread[...], axis=1, keepdims=True)
    sp[...] = jnp.broadcast_to(slot, spread.shape).astype(I32).astype(I16)


def join_table(device, me, key_slot, perm):
    first = device * 4
    owner = (key_slot[pl.ds(first, 4), :] >> 11).astype(F32)
    across = jnp.concatenate([owner[j : j + 1] for j in range(4)], axis=1)
    down = jnp.concatenate([owner, owner], axis=0).T
    index = iota((LANES, KEY_DEV), 1)
    for j in range(4):
        column = down[:, j : j + 1]
        earlier = index < iota((LANES, KEY_DEV), 0) + j * LANES
        same = jnp.where((column == across) & earlier, 1.0, 0.0)
        rank = jnp.sum(same, axis=1, keepdims=True).astype(I32)
        step = (me - column.astype(I32)) & (MEMBERS - 1)
        perm[j * LANES : (j + 1) * LANES, :] = onehot(step * KPP + rank == index)


def fused(
    heavy, keys, heavy_row, key_slot_hbm, measures_hbm, orders_hbm,
    result, report, slot_rows,
    key_slot, measures, pairs, orders, slots, heavy_spot, seg, places, packed, scales, ranks_hist, heavy_hist, meta,
    send, got, side, got_side, acc, sp, spread, local, rank, perm,
    out2, in2, out3, in3, totals, hist,
    hv_sums, hv_in, hm_out, hm_in, slot_out, slot_in,
    local_sem, s_main, r_main, s_side, r_side, s_two, r_two, s_three, r_three,
    s_hv, r_hv, s_hm, r_hm, s_slot, r_slot,
):
    me_x, me_y = lax.axis_index("gx"), lax.axis_index("gy")
    device = me_x * GY + me_y
    me, group = member_of(device)
    barrier = pltpu.get_barrier_semaphore()
    fetch_slots = pltpu.make_async_copy(key_slot_hbm, key_slot, local_sem.at[2])
    fetch_slots.start()
    fetch = pltpu.make_async_copy(measures_hbm, measures, local_sem.at[0])
    fetch.start()
    fetch_orders = pltpu.make_async_copy(orders_hbm, orders, local_sem.at[1])
    fetch_orders.start()

    def place(member, its_group):
        x, y = member >> 4, (member >> 2) & 3
        return (x * 8 + its_group * 2 + ((member >> 1) & 1)) * 2 + (member & 1), y

    def along(s):
        return lax.rem(me + s, MEMBERS)

    def in_group(s):
        return place(along(s), group)

    def across(s):
        return place(me, lax.rem(group + s, GROUPS))

    opposite = (me, group)
    alone = group == me_y

    def copy(src, dst, send_sem, recv_sem, s, target):
        return pltpu.make_async_remote_copy(
            src_ref=src, dst_ref=dst, send_sem=send_sem.at[s], recv_sem=recv_sem.at[s],
            device_id=target, device_id_type=MESH,
        )

    def main_copy(s):
        return copy(send.at[s], got.at[s], s_main, r_main, s, in_group(s))

    def side_copy(s):
        return copy(side.at[s], got_side.at[s], s_side, r_side, s, in_group(s))

    def heavy_copy(s):
        return copy(hv_sums.at[lax.rem(group + s, GROUPS)], hv_in.at[s], s_hv, r_hv, s, across(s))

    def member_copy(s):
        return copy(hm_out.at[along(s)], hm_in.at[s], s_hm, r_hm, s, in_group(s))

    def two_copy(s):
        return copy(out2.at[s], in2.at[s], s_two, r_two, s, across(s))

    def three_copy(s):
        return copy(out3.at[along(s)], in3.at[s], s_three, r_three, s, in_group(s))

    def slot_copy():
        return copy(slot_out, slot_in, s_slot, r_slot, 0, opposite)

    for s in range(1, MEMBERS):
        pl.semaphore_signal(barrier, inc=1, device_id=in_group(s), device_id_type=MESH)

    for s in range(1, GROUPS):
        pl.semaphore_signal(barrier, inc=1, device_id=across(s), device_id_type=MESH)

    @pl.when(jnp.logical_not(alone))
    def _():
        pl.semaphore_signal(barrier, inc=1, device_id=opposite, device_id_type=MESH)

    def pair_sums(count, spots):
        total = jnp.zeros((count, 2 * LANES), F32)
        for b in range(ROWS // BLOCK):
            span = slice(b * BLOCK, (b + 1) * BLOCK)
            total = total + dot(hot16(count, spread16(spots(span))), pairs[span, :])
        return total

    fetch_slots.wait()
    find_slots(keys, heavy_row, key_slot, slots, heavy_spot, ranks_hist, heavy_hist)
    fetch.wait()
    find_ranks(me, slots, heavy_spot, seg, places, ranks_hist, measures, pairs)

    @pl.when(alone)
    def _():
        pl.semaphore_wait(barrier, MEMBERS - 1 + GROUPS - 1)

    @pl.when(jnp.logical_not(alone))
    def _():
        pl.semaphore_wait(barrier, MEMBERS + GROUPS - 1)

    left = iota((1, LANES), 1) < CAPK
    lane = iota((HALF, LANES), 1) & (CAPK - 1)
    lower_lane = lane == iota((HALF, LANES), 0)
    upper_lane = lane == iota((HALF, LANES), 0) + HALF

    def start_sides(c):
        for i in range(STEPS):
            s = c * STEPS + i
            side[s] = jnp.where(left, packed[pl.ds(s, 1), :], scales[s])

        @pl.loop(jnp.maximum(c * STEPS, 1), (c + 1) * STEPS)
        def _(s):
            side_copy(s).start()

    @pl.loop(0, CHUNKS)
    def _(c):
        total = pair_sums(CHUNK, lambda span: seg[:, span] - c * CHUNK)
        lower, lower_power = power_of(total[:, :LANES])
        upper, upper_power = power_of(total[:, LANES:])
        for i in range(STEPS):
            s = c * STEPS + i
            at = slice(i * HALF, (i + 1) * HALF)
            powers = jnp.where(lower_lane, lower_power[at], 0.0)
            powers = powers + jnp.where(upper_lane, upper_power[at], 0.0)
            send[s, 0:HALF] = lower[at].astype(I16)
            send[s, HALF:CAPK] = upper[at].astype(I16)
            scales[s] = jnp.exp2(jnp.sum(powers, axis=0, keepdims=True))

        @pl.loop(jnp.maximum(c * STEPS, 1), (c + 1) * STEPS)
        def _(s):
            main_copy(s).start()

        @pl.when(c == DESCRIBED)
        def _():
            describe(me, slots, places, meta, packed)
            for n in range(DESCRIBED):
                start_sides(n)
            got[0] = send[0]

        @pl.when(c >= DESCRIBED)
        def _():
            start_sides(c)

        @pl.when(c == DESCRIBED + 1)
        def _():
            both = pair_sums(
                MEMBERS * GROUPS,
                lambda span: jnp.where(heavy_spot[:, span] < 0, -1, heavy_spot[:, span] >> 1),
            )
            for n in range(GROUPS):
                at = slice(n * MEMBERS, (n + 1) * MEMBERS)
                hv_sums[n, 0:MEMBERS] = both[at, :LANES]
                hv_sums[n, MEMBERS:HPG] = both[at, LANES:]
                hv_sums[n, HPG : HPG + 8] = jnp.broadcast_to(heavy_hist[n : n + 1, :], (8, LANES))

        @pl.when(c == DESCRIBED + 2)
        def _():
            for s in range(1, GROUPS):
                heavy_copy(s).start()

    got_side[0] = side[0]
    owner_table(me, key_slot, local, rank, spread, sp)

    total = hv_sums[group]
    for s in range(1, GROUPS):
        heavy_copy(s).wait_recv()
        total = total + hv_in[s]
    for m in range(MEMBERS):
        rows = [total[h * MEMBERS + m : h * MEMBERS + m + 1] for h in range(HPD)]
        rows.append(total[HPG : HPG + 2])
        hm_out[m] = jnp.concatenate(rows, axis=0)
    join_table(device, me, key_slot, perm)

    @pl.loop(1, MEMBERS)
    def _(s):
        member_copy(s).start()

    acc[...] = jnp.zeros(acc.shape, F32)
    hist[...] = jnp.zeros(hist.shape, F32)

    @pl.loop(0, MEMBERS // TAKEN)
    def _(g):
        @pl.loop(jnp.maximum(g * TAKEN, 1), (g + 1) * TAKEN)
        def _(s):
            main_copy(s).wait_recv()
            side_copy(s).wait_recv()

        hots, wanted, counts = [], [], []
        for j in range(TAKEN // 2):
            s = g * TAKEN + 2 * j
            a, b = got_side[s], got_side[s + 1]
            entry = jnp.where(left, a, pltpu.roll(b, CAPK, 1)).astype(I32)
            slot = jnp.where(entry >= OWN, entry & (OWN - 1), -1)
            wanted.append(slot)
            counts.append((entry >> 11).astype(F32))
            target = jnp.broadcast_to(slot, (16, LANES)).astype(I16)
            one = value16(jnp.where(left, pltpu.roll(a, CAPK, 1), b))
            zero = jnp.zeros((16, LANES), BF16)
            hots.append(
                jnp.concatenate(
                    [
                        jnp.where(sp[16 * t : 16 * t + 16, :] == target, one, zero)
                        for t in range(OWN // 16)
                    ],
                    axis=0,
                )
            )
        rows = got[pl.ds(g * TAKEN, TAKEN)].reshape(TAKEN * CAPK, LANES).astype(I32)
        low = rows & 255
        pieces = [(rows - low).astype(F32).astype(BF16), low.astype(F32).astype(BF16)]
        found = dot(jnp.concatenate(hots, axis=1), jnp.concatenate(pieces, axis=1))
        acc[...] += found[:, :LANES] + found[:, LANES:]
        slot = jnp.concatenate(wanted, axis=1)
        count = value16(jnp.concatenate(counts, axis=1))
        hist[...] += dot(
            hot16(OWN_ROWS, spread16(slot >> 7)), hot16(LANES, spread16(slot & 127), count), NT
        )

    def part_of(q):
        return pl.ds(pl.multiple_of(q * KEY_DEV, KEY_DEV), KEY_DEV)

    slot_total = hist[...]
    order = (2, 1, 3)
    for n, s in enumerate(order):
        fixed, exponents = encode(acc[part_of(lax.rem(group + s, GROUPS)), :])
        extra = jnp.concatenate(
            [slot_total, *exponents, jnp.zeros((EXTRA - OWN_ROWS - 4, LANES), F32)], axis=0
        )
        out2[s, KEY_DEV : KEY_DEV + EXTRA] = extra.astype(I32).astype(I16)
        out2[s, 0:KEY_DEV] = fixed.astype(I16)
        if n > 0:
            two_copy(order[n - 1]).start()
    slot = sp[part_of(group), :].astype(I32)
    totals[...] = acc[part_of(group), :]
    two_copy(order[-1]).start()
    hm_in[0] = hm_out[me]

    @pl.loop(1, MEMBERS)
    def _(s):
        main_copy(s).wait_send()
        side_copy(s).wait_send()
        member_copy(s).wait_send()
        member_copy(s).wait_recv()

    heavy_total = jnp.sum(hm_in[...], axis=0)
    for s in (1, 3, 2):
        two_copy(s).wait_recv()
        part = in2[s, KEY_DEV : KEY_DEV + EXTRA].astype(I32).astype(F32)
        slot_total = slot_total + part[0:OWN_ROWS]
        for j in range(4):
            at = slice(j * LANES, (j + 1) * LANES)
            scale = scales_down(part[OWN_ROWS + j : OWN_ROWS + 1 + j], LANES, 0)
            totals[at, :] += in2[s, at].astype(I32).astype(F32) * scale
    hist[...] = slot_total
    slot_out[...] = hist[pl.ds(group * 4, 4), :]
    wide = jnp.zeros((KEY_DEV, LANES), F32)
    for r in range(OWN_ROWS):
        wide = wide + jnp.where(slot >> 7 == r, slot_total[r : r + 1], 0.0)
    wide = jnp.where((slot & 127) == iota((KEY_DEV, LANES), 1), wide, 0.0)
    count = jnp.sum(wide, axis=1, keepdims=True)
    totals[...] = totals[...] * (lax.rsqrt(1.0 + count) * (1.0 / FULL))
    for m in range(MEMBERS):
        out3[m] = totals[m * KPP : (m + 1) * KPP, :]
    in3[0] = totals[pl.ds(pl.multiple_of(me * KPP, KPP), KPP), :]
    lane = iota((1, LANES), 1)
    sized = []
    for h in range(HPD):
        number = jnp.sum(
            jnp.where(lane == me * HPD + h, heavy_total[HPD : HPD + 1], 0.0),
            axis=1, keepdims=True,
        )
        sized.append(heavy_total[h : h + 1] * lax.rsqrt(1.0 + number))

    for s in FAR_FIRST:
        three_copy(s).start()

    @pl.when(alone)
    def _():
        slot_rows[...] = slot_out[...]

    @pl.when(jnp.logical_not(alone))
    def _():
        slot_copy().start()

    line = iota((KEY_DEV, LANES), 0)
    fetch_orders.wait()
    attributes = orders[...].astype(F32)
    heavy_part = jnp.zeros((KEY_DEV, LANES), F32)
    lines = []
    for h in range(HPD):
        spot = heavy[device * HPD + h] - device * KEY_DEV
        here = line == spot
        heavy_part = heavy_part + jnp.where(here, sized[h], 0.0)
        lines.append(jnp.sum(jnp.where(here, attributes, 0.0), axis=0, keepdims=True) * sized[h])
    report[...] = jnp.concatenate(lines, axis=0).astype(BF16)
    totals[...] = heavy_part
    for s in range(1, GROUPS):
        two_copy(s).wait_send()
        heavy_copy(s).wait_send()

    @pl.when(jnp.logical_not(alone))
    def _():
        slot_copy().wait_send()
        slot_copy().wait_recv()
        slot_rows[...] = slot_in[...]

    @pl.loop(1, MEMBERS)
    def _(s):
        three_copy(s).wait_recv()

    rows = in3[...].reshape(KEY_DEV, LANES)
    high = rows.astype(BF16)
    low = (rows - high.astype(F32)).astype(BF16)
    both = dot(perm[...], jnp.concatenate([high, low], axis=1))
    found = both[:, :LANES] + both[:, LANES:] + totals[...]
    result[...] = (orders[...].astype(F32) * found).astype(BF16)

    @pl.loop(1, MEMBERS)
    def _(s):
        three_copy(s).wait_send()


def hand_on(*refs):
    half = len(refs) // 2
    for source, target in zip(refs[:half], refs[half:]):
        target[...] = source[...]


def shaped(*dims, dtype=F32):
    return jax.ShapeDtypeStruct(dims, dtype)


def body(measures, row_keys, orders, heavy_keys, key_slot):
    table = key_slot.reshape(key_slot.shape[0] // LANES, LANES)
    dma = pltpu.SemaphoreType.DMA
    outs = (
        shaped(KEY_DEV, LANES, dtype=BF16),
        shaped(HPD, LANES, dtype=BF16),
        shaped(KEY_DEV // LANES, LANES),
    )
    found = pl.pallas_call(
        fused,
        out_shape=outs,
        in_specs=[SMEM] + [VMEM] * 2 + [ANY] * 3,
        out_specs=(VMEM,) * 3,
        scratch_shapes=[
            pltpu.VMEM((KEY_DEV * MEMBERS * GROUPS // LANES, LANES), I32),
            pltpu.VMEM((ROWS, LANES), BF16),
            pltpu.VMEM((ROWS, 2 * LANES), BF16),
            pltpu.VMEM((KEY_DEV, LANES), BF16),
            pltpu.VMEM((1, ROWS), I32),
            pltpu.VMEM((1, ROWS), I32),
            pltpu.VMEM((1, ROWS), I32),
            pltpu.VMEM((1, ROWS), I32),
            pltpu.VMEM((MEMBERS, LANES), F32),
            pltpu.VMEM((MEMBERS, 1, LANES), F32),
            pltpu.VMEM((512, 256), F32),
            pltpu.VMEM((16, LANES), F32),
            pltpu.VMEM((256, LANES), F32),
            pltpu.VMEM((MEMBERS, CAPK, LANES), I16),
            pltpu.VMEM((MEMBERS, CAPK, LANES), I16),
            pltpu.VMEM((MEMBERS, 1, LANES), F32),
            pltpu.VMEM((MEMBERS, 1, LANES), F32),
            pltpu.VMEM((OWN, LANES), F32),
            pltpu.VMEM((OWN, LANES), I16),
            pltpu.VMEM((OWN, LANES), F32),
            pltpu.VMEM((1024, LANES), F32),
            pltpu.VMEM((1024, LANES), F32),
            pltpu.VMEM((KEY_DEV, KEY_DEV), BF16),
            pltpu.VMEM((GROUPS, KEY_DEV + EXTRA, LANES), I16),
            pltpu.VMEM((GROUPS, KEY_DEV + EXTRA, LANES), I16),
            pltpu.VMEM((MEMBERS, KPP, LANES), F32),
            pltpu.VMEM((MEMBERS, KPP, LANES), F32),
            pltpu.VMEM((KEY_DEV, LANES), F32),
            pltpu.VMEM((OWN_ROWS, LANES), F32),
            pltpu.VMEM((GROUPS, HPG + 8, LANES), F32),
            pltpu.VMEM((GROUPS, HPG + 8, LANES), F32),
            pltpu.VMEM((MEMBERS, 4, LANES), F32),
            pltpu.VMEM((MEMBERS, 4, LANES), F32),
            pltpu.VMEM((4, LANES), F32),
            pltpu.VMEM((4, LANES), F32),
            dma((3,)),
        ]
        + [dma((MEMBERS,))] * 4
        + [dma((GROUPS,))] * 2
        + [dma((MEMBERS,))] * 2
        + [dma((GROUPS,))] * 2
        + [dma((MEMBERS,))] * 2
        + [dma((1,))] * 2,
        compiler_params=pltpu.CompilerParams(
            collective_id=0, has_side_effects=True, vmem_limit_bytes=LIMIT
        ),
    )(heavy_keys, row_keys.reshape(1, ROWS), heavy_keys.reshape(1, -1), table, measures, orders)
    result, report, slot_rows = pl.pallas_call(
        hand_on,
        out_shape=outs,
        in_specs=[VMEM] * 3,
        out_specs=(VMEM,) * 3,
    )(*found)
    return (result, report, slot_rows.reshape(KEY_DEV))


def solution(mesh):
    return jax.shard_map(
        body,
        mesh=mesh,
        in_specs=(P(("gx", "gy"), None), P(("gx", "gy")), P(("gx", "gy"), None), P(), P()),
        out_specs=(P(("gx", "gy"), None), P(("gx", "gy"), None), P(("gx", "gy"))),
        check_vma=False,
    )
```

```python
import functools

import jax
import jax.numpy as jnp
from jax import lax
from jax.experimental import pallas as pl
from jax.experimental.pallas import tpu as pltpu
from jax.sharding import PartitionSpec as P

MESH = pl.DeviceIdType.MESH
LANES = 128
F32 = jnp.float32
BF16 = jnp.bfloat16
I32 = jnp.int32
I16 = jnp.int16
VMEM = pl.BlockSpec(memory_space=pltpu.VMEM)
SMEM = pl.BlockSpec(memory_space=pltpu.SMEM)
ANY = pl.BlockSpec(memory_space=pl.ANY)
LIMIT = 60 * 1024 * 1024
NN = (((1,), (0,)), ((), ()))
NT = (((1,), (1,)), ((), ()))

GX, GY = 64, 4
MEMBERS, GROUPS = 64, 4
ROWS = 8192
BLOCK = 2048
CAPK = 64
OWN = 2048
OWN_ROWS = OWN // 128
KEY_DEV = 512
KPP = 8
HPD = 2
HPG = HPD * MEMBERS
STEPS = 8
TAKEN = 8
HALF = CAPK // 2
CHUNK = STEPS * HALF
CHUNKS = MEMBERS // STEPS
DESCRIBED = 1 if STEPS == 8 else 0
EXTRA = 32
FULL = 32000.0


def hops(s):
    return sum(min(n, 4 - n) for n in (s >> 4, (s >> 2) & 3)) + ((s >> 1) & 1)


FAR_FIRST = sorted(range(1, MEMBERS), key=lambda s: -hops(s))


def dot(a, b, dims=NN):
    return lax.dot_general(a, b, dims, preferred_element_type=F32)


def iota(shape, dim):
    return lax.broadcasted_iota(I32, shape, dim)


def onehot(mask):
    return jnp.where(mask, 1.0, 0.0).astype(BF16)


def spread16(row):
    wide = jnp.broadcast_to(row, (16, row.shape[1])) - iota((16, row.shape[1]), 0)
    return wide.astype(I16)


def hot16(count, base, value=None):
    one = jnp.ones(base.shape, BF16) if value is None else value
    zero = jnp.zeros(base.shape, BF16)
    tiles = [jnp.where(base == jnp.int16(16 * t), one, zero) for t in range(count // 16)]
    return jnp.concatenate(tiles, axis=0)


def value16(row):
    return jnp.broadcast_to(row, (16, row.shape[1])).astype(BF16)


def pick(wide, mask):
    return jnp.sum(jnp.where(mask, wide, 0.0), axis=0, keepdims=True)


def power_of(values):
    largest = jnp.max(jnp.abs(values), axis=1, keepdims=True)
    exponent = jnp.ceil(jnp.log2(jnp.maximum(largest, 1e-30)))
    return jnp.round(values * (jnp.exp2(-exponent) * FULL)).astype(I32), exponent


def encode(values):
    fixed, exponent = power_of(values)
    eye = iota((LANES, LANES), 0) == iota((LANES, LANES), 1)
    across = [
        jnp.sum(jnp.where(eye, exponent[at : at + LANES], 0.0), axis=0, keepdims=True)
        for at in range(0, values.shape[0], LANES)
    ]
    return fixed, across


def scales_down(across, count, first):
    shape = (count, LANES)
    mask = iota(shape, 1) == iota(shape, 0) + first
    column = jnp.sum(jnp.where(mask, across, 0.0), axis=1, keepdims=True)
    return jnp.exp2(column) * (1.0 / FULL)


def member_of(block):
    member = (block >> 6) * 16 + (block & 3) * 4 + ((block >> 3) & 1) * 2 + ((block >> 2) & 1)
    return member, (block >> 4) & 3


def find_slots(keys, heavy, key_slot, slots, heavy_spot, hist, heavy_hist):
    hk = heavy[...]
    order = iota((1, hk.shape[1]), 1) & 1
    low = hot16(256, spread16(hk & 255), value16((order + 1).astype(F32)))
    flags = dot(low, hot16(512, spread16(hk >> 8)), NT)
    even = key_slot[pl.ds(0, 512, stride=2), :]
    odd = key_slot[pl.ds(1, 512, stride=2), :]

    def turned(part):
        return jnp.concatenate([part(even).astype(F32).T, part(odd).astype(F32).T], axis=0)

    first = jnp.where(flags > 0.0, -flags, turned(lambda s: s & 255))
    second = turned(lambda s: (s >> 8) - 256)
    table = jnp.concatenate([first, second], axis=0).astype(BF16)
    hist[...] = jnp.zeros(hist.shape, F32)
    heavy_hist[...] = jnp.zeros(heavy_hist.shape, F32)
    low_index = iota((256, BLOCK), 0)

    @pl.loop(0, ROWS // BLOCK)
    def _(b):
        span = pl.ds(pl.multiple_of(b * BLOCK, BLOCK), BLOCK)
        key = keys[:, span]
        wide = dot(table, hot16(512, spread16(key >> 8)))
        mask = low_index == (key & 255)
        part = pick(wide[:256], mask).astype(I32)
        slot = (pick(wide[256:], mask).astype(I32) + 256) * 256 + part
        is_heavy = part < 0
        slot = jnp.where(is_heavy, -1, slot)
        slots[:, span] = slot
        member, group = member_of(key >> 9)
        spot = jnp.where(is_heavy, group * HPG + member * HPD - 1 - part, -1)
        heavy_spot[:, span] = spot
        hist[...] += dot(hot16(512, spread16(slot >> 8)), hot16(256, spread16(slot & 255)), NT)
        heavy_hist[...] += dot(
            hot16(16, spread16(spot >> 7)), hot16(LANES, spread16(spot & 127)), NT
        )


def find_ranks(me, slots, heavy_spot, seg_out, places, hist, measures, pairs):
    present = hist[...] > 0.0
    flag = onehot(present)
    inside = dot(flag, onehot(iota((256, 256), 0) < iota((256, 256), 1)))
    whole = dot(flag, jnp.ones((256, LANES), BF16))
    row, col = iota((512, 512), 0), iota((512, 512), 1)
    before = dot(onehot((col < row) & (col >> 3 == row >> 3)), whole.astype(BF16))
    rank = inside + jnp.concatenate([before, before], axis=1)
    ranks = jnp.where(present, rank, 0.0).T.astype(BF16)
    low_index = iota((256, BLOCK), 0)

    @pl.loop(0, ROWS // BLOCK, unroll=2)
    def _(b):
        span = pl.ds(pl.multiple_of(b * BLOCK, BLOCK), BLOCK)
        slot = slots[:, span]
        light = slot >= 0
        wide = dot(ranks, hot16(512, spread16(slot >> 8)))
        place = pick(wide, low_index == (slot & 255)).astype(I32)
        places[:, span] = jnp.where(light, place, -1)
        step = ((slot >> 11) - me) & (MEMBERS - 1)
        seg_out[:, span] = jnp.where(light, step * HALF + (place & (HALF - 1)), -1)
        bit = jnp.where(light, place >> 5, heavy_spot[:, span] & 1).astype(F32)
        bits = [bit[:, i * LANES : (i + 1) * LANES] for i in range(BLOCK // LANES)]
        down = jnp.concatenate(bits, axis=0).T
        for i in range(BLOCK // LANES):
            at = pl.ds(pl.multiple_of(b * BLOCK + i * LANES, LANES), LANES)
            rows = measures[at, :]
            upper = rows * jnp.broadcast_to(down[:, i : i + 1], (LANES, LANES)).astype(BF16)
            pairs[at, LANES:] = upper
            pairs[at, :LANES] = rows - upper


def describe(me, slots, places, meta, packed):
    meta[...] = jnp.zeros(meta.shape, F32)

    @pl.loop(0, ROWS // BLOCK, unroll=2)
    def _(b):
        span = pl.ds(pl.multiple_of(b * BLOCK, BLOCK), BLOCK)
        slot = slots[:, span]
        base = spread16(places[:, span])
        kinds = jnp.concatenate(
            [
                hot16(64, base),
                hot16(64, base, value16((slot & 255).astype(F32))),
                hot16(64, base, value16(((slot >> 8) & 7).astype(F32))),
            ],
            axis=0,
        )
        step = jnp.where(slot >= 0, ((slot >> 11) - me) & (MEMBERS - 1), -1)
        meta[0:192, :] += dot(kinds, hot16(LANES, spread16(step)), NT)

    turn = meta[...].T
    count, high_sum = turn[:MEMBERS, :LANES], turn[:MEMBERS, LANES:]
    low_sum = pltpu.roll(count, CAPK, 1)
    share = 1.0 / jnp.maximum(count, 1.0)
    low_slot = jnp.floor(low_sum * share + 0.5)
    high_slot = jnp.floor(high_sum * share + 0.5)
    packed[...] = count * OWN + high_slot * 256.0 + low_slot


def owner_table(me, key_slot, local, rank, spread, sp):
    mine_slot = key_slot[...] - me * OWN
    mine = (mine_slot >= 0) & (mine_slot < OWN)
    flag = onehot(mine)
    inside = dot(flag, onehot(iota((LANES, LANES), 0) < iota((LANES, LANES), 1)))
    whole = dot(flag, jnp.ones((LANES, LANES), BF16))
    line = iota(whole.shape, 0) & 3
    for t in range(1, 4):
        inside = inside + jnp.where(line >= t, pltpu.roll(whole, t, 0), 0.0)
    rank[...] = jnp.where(mine, inside, -1.0)
    local[...] = mine_slot.astype(F32)
    eight = iota((KPP, LANES), 0).astype(F32)

    @pl.loop(0, GX, unroll=4)
    def _(x):
        at = pl.ds(pl.multiple_of(x * 16, 16), 16)
        ranks, locals_ = rank[at, :], local[at, :]
        for y in range(GY):
            acc = jnp.zeros((KPP, LANES), F32)
            for j in range(4):
                n = y * 4 + j
                acc = acc + jnp.where(eight == ranks[n : n + 1], locals_[n : n + 1], 0.0)
            first = ((x >> 2) & 3) * KEY_DEV
            first = first + ((x >> 4) * 16 + y * 4 + ((x >> 1) & 1) * 2 + (x & 1)) * KPP
            spread[pl.ds(pl.multiple_of(first, KPP), KPP), :] = acc

    slot = jnp.sum(spread[...], axis=1, keepdims=True)
    sp[...] = jnp.broadcast_to(slot, spread.shape).astype(I32).astype(I16)


def join_table(device, me, key_slot, perm):
    first = device * 4
    owner = (key_slot[pl.ds(first, 4), :] >> 11).astype(F32)
    across = jnp.concatenate([owner[j : j + 1] for j in range(4)], axis=1)
    down = jnp.concatenate([owner, owner], axis=0).T
    index = iota((LANES, KEY_DEV), 1)
    for j in range(4):
        column = down[:, j : j + 1]
        earlier = index < iota((LANES, KEY_DEV), 0) + j * LANES
        same = jnp.where((column == across) & earlier, 1.0, 0.0)
        rank = jnp.sum(same, axis=1, keepdims=True).astype(I32)
        step = (me - column.astype(I32)) & (MEMBERS - 1)
        perm[j * LANES : (j + 1) * LANES, :] = onehot(step * KPP + rank == index)


def fused(
    heavy, keys, heavy_row, key_slot_hbm, measures_hbm, orders_hbm,
    result, report, slot_rows,
    key_slot, measures, pairs, orders, slots, heavy_spot, seg, places, packed, scales, ranks_hist, heavy_hist, meta,
    send, got, side, got_side, acc, sp, spread, local, rank, perm,
    out2, in2, out3, in3, totals, hist,
    hv_sums, hv_in, hm_out, hm_in, slot_out, slot_in,
    local_sem, s_main, r_main, s_side, r_side, s_two, r_two, s_three, r_three,
    s_hv, r_hv, s_hm, r_hm, s_slot, r_slot,
):
    me_x, me_y = lax.axis_index("gx"), lax.axis_index("gy")
    device = me_x * GY + me_y
    me, group = member_of(device)
    barrier = pltpu.get_barrier_semaphore()
    fetch_slots = pltpu.make_async_copy(key_slot_hbm, key_slot, local_sem.at[2])
    fetch_slots.start()
    fetch = pltpu.make_async_copy(measures_hbm, measures, local_sem.at[0])
    fetch.start()
    fetch_orders = pltpu.make_async_copy(orders_hbm, orders, local_sem.at[1])
    fetch_orders.start()

    def place(member, its_group):
        x, y = member >> 4, (member >> 2) & 3
        return (x * 8 + its_group * 2 + ((member >> 1) & 1)) * 2 + (member & 1), y

    def along(s):
        return lax.rem(me + s, MEMBERS)

    def in_group(s):
        return place(along(s), group)

    def across(s):
        return place(me, lax.rem(group + s, GROUPS))

    opposite = (me, group)
    alone = group == me_y

    def copy(src, dst, send_sem, recv_sem, s, target):
        return pltpu.make_async_remote_copy(
            src_ref=src, dst_ref=dst, send_sem=send_sem.at[s], recv_sem=recv_sem.at[s],
            device_id=target, device_id_type=MESH,
        )

    def main_copy(s):
        return copy(send.at[s], got.at[s], s_main, r_main, s, in_group(s))

    def side_copy(s):
        return copy(side.at[s], got_side.at[s], s_side, r_side, s, in_group(s))

    def heavy_copy(s):
        return copy(hv_sums.at[lax.rem(group + s, GROUPS)], hv_in.at[s], s_hv, r_hv, s, across(s))

    def member_copy(s):
        return copy(hm_out.at[along(s)], hm_in.at[s], s_hm, r_hm, s, in_group(s))

    def two_copy(s):
        return copy(out2.at[s], in2.at[s], s_two, r_two, s, across(s))

    def three_copy(s):
        return copy(out3.at[along(s)], in3.at[s], s_three, r_three, s, in_group(s))

    def slot_copy():
        return copy(slot_out, slot_in, s_slot, r_slot, 0, opposite)

    for s in range(1, MEMBERS):
        pl.semaphore_signal(barrier, inc=1, device_id=in_group(s), device_id_type=MESH)

    for s in range(1, GROUPS):
        pl.semaphore_signal(barrier, inc=1, device_id=across(s), device_id_type=MESH)

    @pl.when(jnp.logical_not(alone))
    def _():
        pl.semaphore_signal(barrier, inc=1, device_id=opposite, device_id_type=MESH)

    def pair_sums(count, spots):
        total = jnp.zeros((count, 2 * LANES), F32)
        for b in range(ROWS // BLOCK):
            span = slice(b * BLOCK, (b + 1) * BLOCK)
            total = total + dot(hot16(count, spread16(spots(span))), pairs[span, :])
        return total

    fetch_slots.wait()
    find_slots(keys, heavy_row, key_slot, slots, heavy_spot, ranks_hist, heavy_hist)
    fetch.wait()
    find_ranks(me, slots, heavy_spot, seg, places, ranks_hist, measures, pairs)

    @pl.when(alone)
    def _():
        pl.semaphore_wait(barrier, MEMBERS - 1 + GROUPS - 1)

    @pl.when(jnp.logical_not(alone))
    def _():
        pl.semaphore_wait(barrier, MEMBERS + GROUPS - 1)

    left = iota((1, LANES), 1) < CAPK
    lane = iota((HALF, LANES), 1) & (CAPK - 1)
    lower_lane = lane == iota((HALF, LANES), 0)
    upper_lane = lane == iota((HALF, LANES), 0) + HALF

    def start_sides(c):
        for i in range(STEPS):
            s = c * STEPS + i
            side[s] = jnp.where(left, packed[pl.ds(s, 1), :], scales[s])

        @pl.loop(jnp.maximum(c * STEPS, 1), (c + 1) * STEPS)
        def _(s):
            side_copy(s).start()

    @pl.loop(0, CHUNKS)
    def _(c):
        total = pair_sums(CHUNK, lambda span: seg[:, span] - c * CHUNK)
        lower, lower_power = power_of(total[:, :LANES])
        upper, upper_power = power_of(total[:, LANES:])
        for i in range(STEPS):
            s = c * STEPS + i
            at = slice(i * HALF, (i + 1) * HALF)
            powers = jnp.where(lower_lane, lower_power[at], 0.0)
            powers = powers + jnp.where(upper_lane, upper_power[at], 0.0)
            send[s, 0:HALF] = lower[at].astype(I16)
            send[s, HALF:CAPK] = upper[at].astype(I16)
            scales[s] = jnp.exp2(jnp.sum(powers, axis=0, keepdims=True))

        @pl.loop(jnp.maximum(c * STEPS, 1), (c + 1) * STEPS)
        def _(s):
            main_copy(s).start()

        @pl.when(c == DESCRIBED)
        def _():
            describe(me, slots, places, meta, packed)
            for n in range(DESCRIBED):
                start_sides(n)
            got[0] = send[0]

        @pl.when(c >= DESCRIBED)
        def _():
            start_sides(c)

        @pl.when(c == DESCRIBED + 1)
        def _():
            both = pair_sums(
                MEMBERS * GROUPS,
                lambda span: jnp.where(heavy_spot[:, span] < 0, -1, heavy_spot[:, span] >> 1),
            )
            for n in range(GROUPS):
                at = slice(n * MEMBERS, (n + 1) * MEMBERS)
                hv_sums[n, 0:MEMBERS] = both[at, :LANES]
                hv_sums[n, MEMBERS:HPG] = both[at, LANES:]
                hv_sums[n, HPG : HPG + 8] = jnp.broadcast_to(heavy_hist[n : n + 1, :], (8, LANES))

        @pl.when(c == DESCRIBED + 2)
        def _():
            for s in range(1, GROUPS):
                heavy_copy(s).start()

    got_side[0] = side[0]
    owner_table(me, key_slot, local, rank, spread, sp)

    total = hv_sums[group]
    for s in range(1, GROUPS):
        heavy_copy(s).wait_recv()
        total = total + hv_in[s]
    for m in range(MEMBERS):
        rows = [total[h * MEMBERS + m : h * MEMBERS + m + 1] for h in range(HPD)]
        rows.append(total[HPG : HPG + 2])
        hm_out[m] = jnp.concatenate(rows, axis=0)
    join_table(device, me, key_slot, perm)

    @pl.loop(1, MEMBERS)
    def _(s):
        member_copy(s).start()

    acc[...] = jnp.zeros(acc.shape, F32)
    hist[...] = jnp.zeros(hist.shape, F32)

    @pl.loop(0, MEMBERS // TAKEN)
    def _(g):
        @pl.loop(jnp.maximum(g * TAKEN, 1), (g + 1) * TAKEN)
        def _(s):
            main_copy(s).wait_recv()
            side_copy(s).wait_recv()

        hots, wanted, counts = [], [], []
        for j in range(TAKEN // 2):
            s = g * TAKEN + 2 * j
            a, b = got_side[s], got_side[s + 1]
            entry = jnp.where(left, a, pltpu.roll(b, CAPK, 1)).astype(I32)
            slot = jnp.where(entry >= OWN, entry & (OWN - 1), -1)
            wanted.append(slot)
            counts.append((entry >> 11).astype(F32))
            target = jnp.broadcast_to(slot, (16, LANES)).astype(I16)
            one = value16(jnp.where(left, pltpu.roll(a, CAPK, 1), b))
            zero = jnp.zeros((16, LANES), BF16)
            hots.append(
                jnp.concatenate(
                    [
                        jnp.where(sp[16 * t : 16 * t + 16, :] == target, one, zero)
                        for t in range(OWN // 16)
                    ],
                    axis=0,
                )
            )
        rows = got[pl.ds(g * TAKEN, TAKEN)].reshape(TAKEN * CAPK, LANES).astype(I32)
        low = rows & 255
        pieces = [(rows - low).astype(F32).astype(BF16), low.astype(F32).astype(BF16)]
        found = dot(jnp.concatenate(hots, axis=1), jnp.concatenate(pieces, axis=1))
        acc[...] += found[:, :LANES] + found[:, LANES:]
        slot = jnp.concatenate(wanted, axis=1)
        count = value16(jnp.concatenate(counts, axis=1))
        hist[...] += dot(
            hot16(OWN_ROWS, spread16(slot >> 7)), hot16(LANES, spread16(slot & 127), count), NT
        )

    def part_of(q):
        return pl.ds(pl.multiple_of(q * KEY_DEV, KEY_DEV), KEY_DEV)

    slot_total = hist[...]
    order = (2, 1, 3)
    for n, s in enumerate(order):
        fixed, exponents = encode(acc[part_of(lax.rem(group + s, GROUPS)), :])
        extra = jnp.concatenate(
            [slot_total, *exponents, jnp.zeros((EXTRA - OWN_ROWS - 4, LANES), F32)], axis=0
        )
        out2[s, KEY_DEV : KEY_DEV + EXTRA] = extra.astype(I32).astype(I16)
        out2[s, 0:KEY_DEV] = fixed.astype(I16)
        if n > 0:
            two_copy(order[n - 1]).start()
    slot = sp[part_of(group), :].astype(I32)
    totals[...] = acc[part_of(group), :]
    two_copy(order[-1]).start()
    hm_in[0] = hm_out[me]

    @pl.loop(1, MEMBERS)
    def _(s):
        member_copy(s).wait_recv()

    heavy_total = jnp.sum(hm_in[...], axis=0)
    for s in (1, 3, 2):
        two_copy(s).wait_recv()
        part = in2[s, KEY_DEV : KEY_DEV + EXTRA].astype(I32).astype(F32)
        slot_total = slot_total + part[0:OWN_ROWS]
        for j in range(4):
            at = slice(j * LANES, (j + 1) * LANES)
            scale = scales_down(part[OWN_ROWS + j : OWN_ROWS + 1 + j], LANES, 0)
            totals[at, :] += in2[s, at].astype(I32).astype(F32) * scale
    hist[...] = slot_total
    slot_out[...] = hist[pl.ds(group * 4, 4), :]
    wide = jnp.zeros((KEY_DEV, LANES), F32)
    for r in range(OWN_ROWS):
        wide = wide + jnp.where(slot >> 7 == r, slot_total[r : r + 1], 0.0)
    wide = jnp.where((slot & 127) == iota((KEY_DEV, LANES), 1), wide, 0.0)
    count = jnp.sum(wide, axis=1, keepdims=True)
    totals[...] = totals[...] * (lax.rsqrt(1.0 + count) * (1.0 / FULL))
    for m in range(MEMBERS):
        out3[m] = totals[m * KPP : (m + 1) * KPP, :]
    in3[0] = totals[pl.ds(pl.multiple_of(me * KPP, KPP), KPP), :]
    lane = iota((1, LANES), 1)
    sized = []
    for h in range(HPD):
        number = jnp.sum(
            jnp.where(lane == me * HPD + h, heavy_total[HPD : HPD + 1], 0.0),
            axis=1, keepdims=True,
        )
        sized.append(heavy_total[h : h + 1] * lax.rsqrt(1.0 + number))

    for s in FAR_FIRST:
        three_copy(s).start()

    @pl.when(alone)
    def _():
        slot_rows[...] = slot_out[...]

    @pl.when(jnp.logical_not(alone))
    def _():
        slot_copy().start()

    @pl.loop(1, MEMBERS)
    def _(s):
        main_copy(s).wait_send()
        side_copy(s).wait_send()
        member_copy(s).wait_send()

    line = iota((KEY_DEV, LANES), 0)
    fetch_orders.wait()
    attributes = orders[...].astype(F32)
    heavy_part = jnp.zeros((KEY_DEV, LANES), F32)
    lines = []
    for h in range(HPD):
        spot = heavy[device * HPD + h] - device * KEY_DEV
        here = line == spot
        heavy_part = heavy_part + jnp.where(here, sized[h], 0.0)
        lines.append(jnp.sum(jnp.where(here, attributes, 0.0), axis=0, keepdims=True) * sized[h])
    report[...] = jnp.concatenate(lines, axis=0).astype(BF16)
    totals[...] = heavy_part
    for s in range(1, GROUPS):
        two_copy(s).wait_send()
        heavy_copy(s).wait_send()

    @pl.when(jnp.logical_not(alone))
    def _():
        slot_copy().wait_send()
        slot_copy().wait_recv()
        slot_rows[...] = slot_in[...]

    @pl.loop(1, MEMBERS)
    def _(s):
        three_copy(s).wait_recv()

    rows = in3[...].reshape(KEY_DEV, LANES)
    high = rows.astype(BF16)
    low = (rows - high.astype(F32)).astype(BF16)
    both = dot(perm[...], jnp.concatenate([high, low], axis=1))
    found = both[:, :LANES] + both[:, LANES:] + totals[...]
    result[...] = (orders[...].astype(F32) * found).astype(BF16)

    @pl.loop(1, MEMBERS)
    def _(s):
        three_copy(s).wait_send()


def hand_on(*refs):
    half = len(refs) // 2
    for source, target in zip(refs[:half], refs[half:]):
        target[...] = source[...]


def shaped(*dims, dtype=F32):
    return jax.ShapeDtypeStruct(dims, dtype)


def body(measures, row_keys, orders, heavy_keys, key_slot):
    table = key_slot.reshape(key_slot.shape[0] // LANES, LANES)
    dma = pltpu.SemaphoreType.DMA
    outs = (
        shaped(KEY_DEV, LANES, dtype=BF16),
        shaped(HPD, LANES, dtype=BF16),
        shaped(KEY_DEV // LANES, LANES),
    )
    found = pl.pallas_call(
        fused,
        out_shape=outs,
        in_specs=[SMEM] + [VMEM] * 2 + [ANY] * 3,
        out_specs=(VMEM,) * 3,
        scratch_shapes=[
            pltpu.VMEM((KEY_DEV * MEMBERS * GROUPS // LANES, LANES), I32),
            pltpu.VMEM((ROWS, LANES), BF16),
            pltpu.VMEM((ROWS, 2 * LANES), BF16),
            pltpu.VMEM((KEY_DEV, LANES), BF16),
            pltpu.VMEM((1, ROWS), I32),
            pltpu.VMEM((1, ROWS), I32),
            pltpu.VMEM((1, ROWS), I32),
            pltpu.VMEM((1, ROWS), I32),
            pltpu.VMEM((MEMBERS, LANES), F32),
            pltpu.VMEM((MEMBERS, 1, LANES), F32),
            pltpu.VMEM((512, 256), F32),
            pltpu.VMEM((16, LANES), F32),
            pltpu.VMEM((256, LANES), F32),
            pltpu.VMEM((MEMBERS, CAPK, LANES), I16),
            pltpu.VMEM((MEMBERS, CAPK, LANES), I16),
            pltpu.VMEM((MEMBERS, 1, LANES), F32),
            pltpu.VMEM((MEMBERS, 1, LANES), F32),
            pltpu.VMEM((OWN, LANES), F32),
            pltpu.VMEM((OWN, LANES), I16),
            pltpu.VMEM((OWN, LANES), F32),
            pltpu.VMEM((1024, LANES), F32),
            pltpu.VMEM((1024, LANES), F32),
            pltpu.VMEM((KEY_DEV, KEY_DEV), BF16),
            pltpu.VMEM((GROUPS, KEY_DEV + EXTRA, LANES), I16),
            pltpu.VMEM((GROUPS, KEY_DEV + EXTRA, LANES), I16),
            pltpu.VMEM((MEMBERS, KPP, LANES), F32),
            pltpu.VMEM((MEMBERS, KPP, LANES), F32),
            pltpu.VMEM((KEY_DEV, LANES), F32),
            pltpu.VMEM((OWN_ROWS, LANES), F32),
            pltpu.VMEM((GROUPS, HPG + 8, LANES), F32),
            pltpu.VMEM((GROUPS, HPG + 8, LANES), F32),
            pltpu.VMEM((MEMBERS, 4, LANES), F32),
            pltpu.VMEM((MEMBERS, 4, LANES), F32),
            pltpu.VMEM((4, LANES), F32),
            pltpu.VMEM((4, LANES), F32),
            dma((3,)),
        ]
        + [dma((MEMBERS,))] * 4
        + [dma((GROUPS,))] * 2
        + [dma((MEMBERS,))] * 2
        + [dma((GROUPS,))] * 2
        + [dma((MEMBERS,))] * 2
        + [dma((1,))] * 2,
        compiler_params=pltpu.CompilerParams(
            collective_id=0, has_side_effects=True, vmem_limit_bytes=LIMIT
        ),
    )(heavy_keys, row_keys.reshape(1, ROWS), heavy_keys.reshape(1, -1), table, measures, orders)
    result, report, slot_rows = pl.pallas_call(
        hand_on,
        out_shape=outs,
        in_specs=[VMEM] * 3,
        out_specs=(VMEM,) * 3,
    )(*found)
    return (result, report, slot_rows.reshape(KEY_DEV))


def solution(mesh):
    return jax.shard_map(
        body,
        mesh=mesh,
        in_specs=(P(("gx", "gy"), None), P(("gx", "gy")), P(("gx", "gy"), None), P(), P()),
        out_specs=(P(("gx", "gy"), None), P(("gx", "gy"), None), P(("gx", "gy"))),
        check_vma=False,
    )
```
